256 devices in a mesh: member: 2 (over y_lo), lat: 8 (over x, core), lon: 16 (over z, y_hi).
Axes of the slice: x: 4, y: 4 (y_hi: 2, y_lo: 2; y = y_hi * 2 + y_lo), z: 8, core: 2. Of those that a mesh axis runs over, the one named last changes fastest.
Arguments:
- fields: float32 [4, 192, 64, 2048], P('member', None, 'lat', 'lon'), parts along dimension 0, may hold values from -6 to 6
- wind_east: float32 [64, 2048], P('lat', 'lon'), may hold values from -0.3 to 0.3
- wind_north: float32 [64, 2048], P('lat', 'lon'), may hold values from -0.3 to 0.3
- diffusion: float32 [64, 2048], P('lat', 'lon'), may hold values from 0.01 to 0.08
- inflow_owner: int32 [2048, 1], P(('lat', 'lon')), may hold values from 0 to 15; in each aligned block of 16 rows (0 to 15, 16 to 31, ...) at most 2 rows name the same one
- inflow_cell: int32 [2048, 128], P(('lat', 'lon')), may hold values from 0 to 1023
- inflow_node: int32 [2048, 128], P(('lat', 'lon')), may hold values from 0 to 255
- inflow_weight: float32 [2048, 128], P(('lat', 'lon')), may hold values from 0.25 to 1.5
- encoder: bfloat16 [192, 512], replicated, may hold values from -0.21875 to 0.21875
- sender_weight: bfloat16 [2, 512, 512], replicated, may hold values from -0.25 to 0.25
- receiver_weight: bfloat16 [2, 512, 512], replicated, may hold values from -0.25 to 0.25
- update_weight: bfloat16 [2, 512, 512], replicated, may hold values from -0.25 to 0.25
- decoder: bfloat16 [512, 192], replicated, may hold values from -0.25 to 0.25
- edge_sender: int32 [8, 16, 1536], P('lat', 'lon'), may hold values from 0 to 447, as said below
- edge_receiver: int32 [8, 16, 1536], P('lat', 'lon'), may hold values from 0 to 255
- halo_rows: int32 [8, 16, 4, 48], P('lat', 'lon'), may hold values from 0 to 255
- outflow_owner: int32 [2048, 1], P(('lat', 'lon')), may hold values from 0 to 15; in each aligned block of 16 rows (0 to 15, 16 to 31, ...) at most 2 rows name the same one
- outflow_node: int32 [2048, 128], P(('lat', 'lon')), may hold values from 0 to 255
- outflow_cell: int32 [2048, 128], P(('lat', 'lon')), may hold values from 0 to 1023
- outflow_weight: float32 [2048, 128], P(('lat', 'lon')), may hold values from 0.25 to 1.5
Outputs:
- revised_outlook: float32 [4, 192, 64, 2048], P('member', None, 'lat', 'lon'), parts along dimension 0
The draws below stay inside these ranges and needn't reach their ends.
There are 2 independent parts, one for each index of `member`. The reference program is written for one: setup_inputs(seed, part) draws one part's arguments, and reference() takes and returns one part's arrays. A program takes and returns all parts, laid end to end along the dimension named above; an argument that names none is the same for every part. Nothing has to cross between parts.
Inputs may be any that keep to these rules, and one draw needn't show every extreme that they name: `inflow_owner`: among the 16 rows of one device, no lon index appears more than 2 times. `outflow_owner`: among the 16 rows of one device, no lon index appears more than 2 times. `edge_sender`: A value below 256 names a node of the edge's own partition; a value 256 + q * 48 + p names halo slot p toward neighbour q as in the reference program. No edge of the first lat index uses q = 0, none of the last uses q = 1.
All inputs are finite; a program needn't handle non-finite values.
Results may differ from the reference program's by a relative error of at most 0.0075.
Values may be sent and summed in bfloat16 or wider, within the bound.
A program may use at most 128 MiB of HBM per device.

```python
import math
import jax
import jax.numpy as jnp
import numpy as np
from jax import lax

BATCH_REALIZATION = 2
POINT_QUANTITIES = 192
PATCH_PARALLELS = 8
PATCH_MERIDIANS = 128
GLOBE_PARALLELS = 64
GLOBE_MERIDIANS = 2048
DSTEPS = 2
BLOCKS = 16
ENTRIES = 128
CAP = 2
ROWS = 2048
NODE_DEV = 256
NODES = 32768
HCAP = 48
EDGES = 1536
HID = 512
LAYERS = 2
N_LAT = 8
N_LON = 16


def draw_edge_sender(key, part):
    base = jax.random.fold_in(key, 41)
    keys = jax.random.split(base, 4)
    shape = (N_LAT, N_LON, EDGES)
    choose_local = jax.random.randint(keys[0], shape, 0, 10)
    local_node = jax.random.randint(keys[1], shape, 0, NODE_DEV)
    quarter = jax.random.randint(keys[2], shape, 0, 4)
    lat_index = jnp.arange(N_LAT, dtype=jnp.int32)[:, None, None]
    missing = (quarter == 0) & (lat_index == 0) | (quarter == 1) & (lat_index == N_LAT - 1)
    quarter = jnp.where(missing, quarter + 2, quarter)
    slot_index = jax.random.randint(keys[3], shape, 0, HCAP)
    result = jnp.where(choose_local < 6, local_node, NODE_DEV + quarter * HCAP + slot_index)
    return result.astype(jnp.int32)


def touch_ends(values, rng, low, high):
    index_at = [jax.random.randint(jax.random.fold_in(rng, axis), (), 0, length) for axis, length in enumerate(values.shape)]
    longest = values.shape.index(max(values.shape))
    neighbour = index_at[:longest] + [(index_at[longest] + 1) % values.shape[longest]] + index_at[longest + 1:]
    return values.at[tuple(index_at)].set(low).at[tuple(neighbour)].set(high)


def shard_levels(rng, extent, pieces, least, high):
    level, own = 1.0, jax.random.fold_in(rng, 6)
    for position, parts in pieces:
        steps = jnp.exp(jax.random.uniform(jax.random.fold_in(own, position), (parts,), jnp.float32, least / len(pieces), high / len(pieces)))
        level = level * jnp.repeat(steps, extent[position] // parts).reshape([-1 if axis == position else 1 for axis in range(len(extent))])
    return level


def shared_out(stream_key, own, number, rows, number_of, top, limit, skew):
    sequence = jax.random.permutation(stream_key, number_of)
    heavy_load, ordinary = load_shares(number_of, rows * top, limit, skew, True), load_shares(number_of, rows * top, limit, skew, False)
    places = jnp.arange(number_of)

    def named(sizes, offset_by):
        used = int((sizes > 0).sum())
        fixed = max(1, used // 4)
        passed = fixed + (places - fixed + offset_by * (used - fixed)) % max(1, number_of - fixed)
        return jnp.zeros((number_of,), jnp.int32).at[sequence[jnp.where(places < fixed, places, passed)]].set(jnp.asarray(sizes, jnp.int32))

    sizes = jnp.where(number % 4 == 0, named(heavy_load, number // 4), named(ordinary, number - number // 4 - 1))
    mixed = jax.random.permutation(jax.random.fold_in(own, 3), number_of)
    source_of, sink = mixed[0:number_of // 2 * 2:2], mixed[1:number_of // 2 * 2:2]
    margin = jnp.minimum(sizes[source_of] - 1, limit - sizes[sink]) // 2
    margin = jnp.where((source_of == sequence[0]) | (sink == sequence[0]) | (sizes[sink] == 0), 0, jnp.maximum(margin, 0))
    passed = jax.random.randint(jax.random.fold_in(own, 4), (number_of // 2,), 0, 1 << 20) % (margin + 1)
    sizes = sizes.at[source_of].add(-passed).at[sink].add(passed)
    labels = jnp.searchsorted(jnp.cumsum(sizes), jnp.arange(rows * top), side="right").astype(jnp.int32)
    grid = labels.reshape(top, rows).T
    grid = grid[jax.random.permutation(jax.random.fold_in(own, 1), rows)]
    offset_by = jax.random.randint(jax.random.fold_in(own, 2), (rows, 1), 0, top)
    return jnp.take_along_axis(grid, (jnp.arange(top)[None, :] + offset_by) % top, axis=1)


def load_shares(amount, total, limit, skew, full):
    loads = [(1 << 20) // math.isqrt(standing ** skew) + 1 for standing in range(1, amount + 1)]
    largest = limit if full else min(limit, max(-(-total // amount), total * loads[0] // sum(loads)))
    least = 1 if total - largest >= amount - 1 else 0
    counts, rest = [largest] + [least] * (amount - 1), total - largest - least * (amount - 1)
    while rest > 0:
        movable = [i for i in range(1, amount) if counts[i] < largest] or [i for i in range(1, amount) if counts[i] < limit]
        mass, budget = sum([loads[i] for i in movable]), rest
        for i in movable:
            extra = min(limit - counts[i], max(1, budget * loads[i] // mass), rest)
            counts[i] = counts[i] + extra
            rest = rest - extra
    return np.array(counts)


def noise(own_key, dims, scale, bound, pieces=(), kind=jnp.bfloat16):
    values = scale * jax.random.normal(own_key, dims, jnp.float32)
    if pieces:
        values = values * shard_levels(own_key, dims, pieces, -0.22, 0.18)
    return jnp.clip(values, -bound, bound).astype(kind)


def setup_inputs(seed: int = 0, part: int = 0) -> dict:
    key_of = jax.random.split(jax.random.key(seed), 21)
    part_keys = jax.random.split(jax.random.fold_in(key_of[20], part), 21)
    fields = noise(part_keys[0], (BATCH_REALIZATION, POINT_QUANTITIES, GLOBE_PARALLELS, GLOBE_MERIDIANS), 1.0, 6.0, ((2, 8), (3, 16)), jnp.float32)
    wind_east = jnp.clip(jax.random.uniform(key_of[1], (GLOBE_PARALLELS, GLOBE_MERIDIANS), jnp.float32, -0.3, 0.3) * shard_levels(key_of[1], (GLOBE_PARALLELS, GLOBE_MERIDIANS), ((0, 8), (1, 16)), -0.4, 0.0), -0.3, 0.3)
    wind_north = jnp.clip(jax.random.uniform(key_of[2], (GLOBE_PARALLELS, GLOBE_MERIDIANS), jnp.float32, -0.3, 0.3) * shard_levels(key_of[2], (GLOBE_PARALLELS, GLOBE_MERIDIANS), ((0, 8), (1, 16)), -0.4, 0.0), -0.3, 0.3)
    diffusion = jnp.clip(jnp.exp(math.log(0.08) - 2.0794415 * jax.random.uniform(key_of[3], (GLOBE_PARALLELS, GLOBE_MERIDIANS), jnp.float32) ** shard_levels(key_of[3], (GLOBE_PARALLELS, GLOBE_MERIDIANS), ((0, 8), (1, 16)), -0.2, 0.2)), 0.01, 0.08)
    inflow_owner_keys = jax.random.split(jax.random.fold_in(key_of[4], 1), ROWS // BLOCKS)
    inflow_owner_turns = jax.random.permutation(jax.random.fold_in(key_of[4], 3), ROWS // BLOCKS)
    inflow_owner = jax.vmap(lambda own, number: shared_out(jax.random.fold_in(key_of[4], 2), own, number, BLOCKS, N_LON, 1, CAP, 2))(inflow_owner_keys, inflow_owner_turns).reshape((ROWS, 1))
    inflow_cell = touch_ends(jax.random.randint(key_of[5], (ROWS, ENTRIES), 0, PATCH_PARALLELS * PATCH_MERIDIANS), jax.random.fold_in(key_of[5], 1), 0, (PATCH_PARALLELS * PATCH_MERIDIANS) - 1).astype(jnp.int32)
    inflow_node = touch_ends(jax.random.randint(key_of[6], (ROWS, ENTRIES), 0, NODE_DEV), jax.random.fold_in(key_of[6], 1), 0, NODE_DEV - 1).astype(jnp.int32)
    inflow_weight = jnp.clip(0.25 + 1.25 * jax.random.uniform(key_of[7], (ROWS, ENTRIES), jnp.float32) ** shard_levels(key_of[7], (ROWS, ENTRIES), ((0, 128),), -0.2, 0.2), 0.25, 1.5)
    encoder = noise(key_of[8], (POINT_QUANTITIES, HID), (4 * POINT_QUANTITIES) ** -0.5, 0.21875)
    sender_weight = noise(key_of[9], (LAYERS, HID, HID), HID ** -0.5, 0.25)
    receiver_weight = noise(key_of[10], (LAYERS, HID, HID), HID ** -0.5, 0.25)
    update_weight = noise(key_of[11], (LAYERS, HID, HID), HID ** -0.5, 0.25)
    decoder = noise(key_of[12], (HID, POINT_QUANTITIES), HID ** -0.5, 0.25)
    edge_sender = draw_edge_sender(jax.random.fold_in(key_of[20], 71), part)
    edge_receiver = touch_ends(jax.random.randint(key_of[14], (N_LAT, N_LON, EDGES), 0, NODE_DEV), jax.random.fold_in(key_of[14], 1), 0, NODE_DEV - 1).astype(jnp.int32)
    halo_rows = touch_ends(jax.random.randint(key_of[15], (N_LAT, N_LON, 4, HCAP), 0, NODE_DEV), jax.random.fold_in(key_of[15], 1), 0, NODE_DEV - 1).astype(jnp.int32)
    outflow_owner_keys = jax.random.split(jax.random.fold_in(key_of[16], 1), ROWS // BLOCKS)
    outflow_owner_turns = jax.random.permutation(jax.random.fold_in(key_of[16], 3), ROWS // BLOCKS)
    outflow_owner = jax.vmap(lambda own, number: shared_out(jax.random.fold_in(key_of[16], 2), own, number, BLOCKS, N_LON, 1, CAP, 2))(outflow_owner_keys, outflow_owner_turns).reshape((ROWS, 1))
    outflow_node = touch_ends(jax.random.randint(key_of[17], (ROWS, ENTRIES), 0, NODE_DEV), jax.random.fold_in(key_of[17], 1), 0, NODE_DEV - 1).astype(jnp.int32)
    outflow_cell = touch_ends(jax.random.randint(key_of[18], (ROWS, ENTRIES), 0, PATCH_PARALLELS * PATCH_MERIDIANS), jax.random.fold_in(key_of[18], 1), 0, (PATCH_PARALLELS * PATCH_MERIDIANS) - 1).astype(jnp.int32)
    outflow_weight = jnp.clip(0.25 + 1.25 * jax.random.uniform(key_of[19], (ROWS, ENTRIES), jnp.float32) ** shard_levels(key_of[19], (ROWS, ENTRIES), ((0, 128),), -0.2, 0.2), 0.25, 1.5)
    return dict(fields=fields, wind_east=wind_east, wind_north=wind_north, diffusion=diffusion, inflow_owner=inflow_owner, inflow_cell=inflow_cell, inflow_node=inflow_node, inflow_weight=inflow_weight, encoder=encoder, sender_weight=sender_weight, receiver_weight=receiver_weight, update_weight=update_weight, decoder=decoder, edge_sender=edge_sender, edge_receiver=edge_receiver, halo_rows=halo_rows, outflow_owner=outflow_owner, outflow_node=outflow_node, outflow_cell=outflow_cell, outflow_weight=outflow_weight)


def advance(extended, east_rate, north_rate, spread):
    middle = extended[:, 1:-1, 1:-1]
    west_cells = extended[:, 1:-1, :-2]
    east_cells = extended[:, 1:-1, 2:]
    south_cells = extended[:, :-2, 1:-1]
    north_cells = extended[:, 2:, 1:-1]
    result = middle - jnp.maximum(east_rate, 0.0) * (middle - west_cells)
    result = result - jnp.minimum(east_rate, 0.0) * (east_cells - middle)
    result = result - jnp.maximum(north_rate, 0.0) * (middle - south_cells)
    result = result - jnp.minimum(north_rate, 0.0) * (north_cells - middle)
    return result + spread * (west_cells + east_cells + south_cells + north_cells - 4.0 * middle)

def normalize(values):
    scale = lax.rsqrt(lax.optimization_barrier(jnp.mean(values * values, axis=-1, keepdims=True)) + 1e-06)
    return (values * scale).astype(jnp.bfloat16)

def reference(fields, wind_east, wind_north, diffusion, inflow_owner, inflow_cell, inflow_node, inflow_weight, encoder, sender_weight, receiver_weight, update_weight, decoder, edge_sender, edge_receiver, halo_rows, outflow_owner, outflow_node, outflow_cell, outflow_weight):
    latent_quantities = BATCH_REALIZATION * POINT_QUANTITIES
    current_condition = fields.reshape(latent_quantities, GLOBE_PARALLELS, GLOBE_MERIDIANS)
    for sub_step in range(DSTEPS):
        extended = jnp.pad(current_condition, ((0, 0), (1, 1), (0, 0)), mode='edge')
        extended = jnp.concatenate([extended[:, :, -1:], extended, extended[:, :, :1]], axis=2)
        current_condition = advance(extended, wind_east, wind_north, diffusion)
    device_count = N_LAT * N_LON
    block_rows = inflow_owner.shape[0]
    device_of = jnp.arange(block_rows, dtype=jnp.int32) // BLOCKS
    lat_of = (device_of // N_LON)[:, None]
    lon_of = (device_of % N_LON)[:, None]
    table = current_condition.reshape(latent_quantities, GLOBE_PARALLELS * GLOBE_MERIDIANS).T
    grid_index = (lat_of * PATCH_PARALLELS + inflow_cell // PATCH_MERIDIANS) * GLOBE_MERIDIANS + lon_of * PATCH_MERIDIANS + inflow_cell % PATCH_MERIDIANS
    inflow = (jnp.take(table, grid_index.reshape(-1).astype(jnp.int32), axis=0) * inflow_weight.reshape(-1, 1)).astype(jnp.bfloat16)
    node_index = ((lat_of * N_LON + inflow_owner) * NODE_DEV + inflow_node).reshape(-1).astype(jnp.int32)
    node_input = jax.ops.segment_sum(inflow.astype(jnp.float32), node_index, num_segments=NODES)
    embedded = node_input.astype(jnp.bfloat16).reshape(NODES * BATCH_REALIZATION, POINT_QUANTITIES)
    hidden = jax.nn.silu(jnp.dot(embedded, encoder, preferred_element_type=jnp.float32))
    lat_step = jnp.array([-1, 1, 0, 0], dtype=jnp.int32)
    lon_step = jnp.array([0, 0, -1, 1], dtype=jnp.int32)
    lat_grid = jnp.arange(N_LAT, dtype=jnp.int32)[:, None, None]
    lon_grid = jnp.arange(N_LON, dtype=jnp.int32)[None, :, None]
    device_grid = lat_grid * N_LON + lon_grid
    is_local = edge_sender < NODE_DEV
    relative = jnp.maximum(edge_sender - NODE_DEV, 0)
    quarter = jnp.clip(relative // HCAP, 0, 3)
    slot_index = relative % HCAP
    near_lat = jnp.clip(lat_grid + lat_step[quarter], 0, N_LAT - 1)
    near_lon = (lon_grid + lon_step[quarter]) % N_LON
    halo_flat = halo_rows.reshape(N_LAT, N_LON, 4 * HCAP)
    halo_node = jnp.take_along_axis(halo_flat, jnp.where(is_local, 0, quarter * HCAP + slot_index).astype(jnp.int32), axis=2)
    sender_global = jnp.where(is_local, device_grid * NODE_DEV + edge_sender, (near_lat * N_LON + near_lon) * NODE_DEV + halo_node)
    sender_global = sender_global.reshape(device_count, EDGES).astype(jnp.int32)
    receiver_local = edge_receiver.reshape(device_count, EDGES).astype(jnp.int32)
    device_ids = jnp.arange(device_count, dtype=jnp.int32)
    for layer in range(LAYERS):
        normed = normalize(hidden)
        source = jnp.dot(normed, sender_weight[layer], preferred_element_type=jnp.float32).astype(jnp.bfloat16).reshape(NODES, BATCH_REALIZATION, HID)
        target = jnp.dot(normed, receiver_weight[layer], preferred_element_type=jnp.float32).reshape(NODES, BATCH_REALIZATION, HID)

        def partition(operands):
            senders, receivers, device = operands
            own_target = lax.dynamic_slice_in_dim(target, (device * NODE_DEV).astype(jnp.int32), NODE_DEV, 0)
            summed = jnp.take(source, senders, axis=0).astype(jnp.float32) + jnp.take(own_target, receivers, axis=0)
            message = jax.nn.silu(summed).astype(jnp.bfloat16)
            return jax.ops.segment_sum(message.astype(jnp.float32), receivers, num_segments=NODE_DEV).astype(jnp.bfloat16)
        collected = lax.map(partition, (sender_global, receiver_local, device_ids))
        collected = collected.reshape(NODES * BATCH_REALIZATION, HID)
        hidden = hidden + jnp.dot(collected, update_weight[layer], preferred_element_type=jnp.float32)
    correction = jnp.dot(normalize(hidden), decoder, preferred_element_type=jnp.float32).astype(jnp.bfloat16).reshape(NODES, latent_quantities)
    source_node = (device_of[:, None] * NODE_DEV + outflow_node).reshape(-1).astype(jnp.int32)
    outflow = (jnp.take(correction, source_node, axis=0).astype(jnp.float32) * outflow_weight.reshape(-1, 1)).astype(jnp.bfloat16)
    cell_index = (lat_of * PATCH_PARALLELS + outflow_cell // PATCH_MERIDIANS) * GLOBE_MERIDIANS + outflow_owner * PATCH_MERIDIANS + outflow_cell % PATCH_MERIDIANS
    add_learned_fix = jax.ops.segment_sum(outflow.astype(jnp.float32), cell_index.reshape(-1).astype(jnp.int32), num_segments=GLOBE_PARALLELS * GLOBE_MERIDIANS)
    revised_outlook = current_condition + add_learned_fix.T.reshape(latent_quantities, GLOBE_PARALLELS, GLOBE_MERIDIANS)
    return revised_outlook.reshape(BATCH_REALIZATION, POINT_QUANTITIES, GLOBE_PARALLELS, GLOBE_MERIDIANS)
```

```python
import jax
import jax.numpy as jnp
from jax import lax
from jax.experimental import pallas as pl
from jax.experimental.pallas import tpu as pltpu
from jax.sharding import PartitionSpec as P

F32, BF16 = jnp.float32, jnp.bfloat16
MESH = pl.DeviceIdType.MESH
MEMBERS = 2
CHANNELS = 192
FEATURES = MEMBERS * CHANNELS
ROWS, COLS = 8, 128
CELLS = ROWS * COLS
BLOCKS, ENTRIES, CAP = 16, 128, 2
NODES = 256
HCAP = 48
EDGES = 1536
HID = 512
LAYERS = 2
N_LAT, N_LON = 8, 16
N_Z = N_LON // 2
GROUP = 48
GROUPS = FEATURES // GROUP
COPIES = 128
VMEM_LIMIT = 66 * 1024 * 1000


def nt_dot(a, b):
    return lax.dot_general(a, b, (((1,), (1,)), ((), ())), preferred_element_type=F32)


def mm(a, b):
    return jnp.dot(a, b, preferred_element_type=F32)


def hot(mask):
    return jnp.where(mask, 1.0, 0.0).astype(BF16)


def silu(v):
    half = 0.5 * v
    return half + half * jnp.tanh(half)


def normalize(values):
    scale = lax.rsqrt(jnp.mean(values * values, axis=-1, keepdims=True) + 1e-06)
    return (values * scale).astype(BF16)


def lanes(shape):
    return lax.broadcasted_iota(jnp.int32, shape, 1)


def sublanes(shape):
    return lax.broadcasted_iota(jnp.int32, shape, 0)


def column(row):
    return jnp.transpose(jnp.broadcast_to(row.astype(F32), (128, 128))).astype(jnp.int32)


def kernel(
    in_source,
    out_source,
    fields_hbm,
    wind_east,
    wind_north,
    diffusion,
    inflow_cell,
    inflow_node,
    inflow_weight,
    encoder_hbm,
    sender_hbm,
    receiver_hbm,
    update_hbm,
    decoder_hbm,
    edge_sender,
    edge_receiver,
    halo_rows,
    outflow_node,
    outflow_cell,
    outflow_weight,
    out_hbm,
    tile,
    state_a,
    state_b,
    lat_out,
    lat_in,
    lon_out,
    lon_in,
    grid_bf,
    cell_hot,
    flow,
    node_hot,
    pack_out,
    pack_in,
    want_in,
    rs_out,
    rs_in,
    rs_y_out,
    rs_y_in,
    rs_last_out,
    rs_last_in,
    node_input,
    edge_hot,
    collect_hot,
    want_hot,
    encoder,
    sender_w,
    receiver_w,
    update_w,
    decoder,
    hidden,
    source_target,
    halo_out,
    halo,
    summed,
    message,
    spread,
    ring,
    ring_y,
    adjust,
    load_sem,
    send_sem,
    recv_sem,
):
    lat = lax.axis_index("lat")
    lon = lax.axis_index("lon")
    z, y = lon // 2, lon % 2
    sides = (
        {"lat": (lat + N_LAT - 1) % N_LAT},
        {"lat": (lat + 1) % N_LAT},
        {"lon": (lon + N_LON - 1) % N_LON},
        {"lon": (lon + 1) % N_LON},
    )
    above = {"lon": (lon + 2) % N_LON}
    below = {"lon": (lon + N_LON - 2) % N_LON}
    partner = {"lon": 2 * z + (1 - y)}
    used = [0]
    started = []

    def copy(src, dst, device):
        index = used[0]
        used[0] += 1
        made = pltpu.make_async_remote_copy(
            src_ref=src,
            dst_ref=dst,
            send_sem=send_sem.at[index],
            recv_sem=recv_sem.at[index],
            device_id=device,
            device_id_type=MESH,
        )
        made.start()
        started.append(made)
        return made

    loads = {}
    for index, (name, src, dst) in enumerate(
        (
            ("fields", fields_hbm, tile),
            ("encoder", encoder_hbm, encoder),
            ("sender", sender_hbm, sender_w),
            ("receiver", receiver_hbm, receiver_w),
            ("update", update_hbm, update_w),
            ("decoder", decoder_hbm, decoder),
        )
    ):
        loads[name] = pltpu.make_async_copy(src, dst, load_sem.at[index])
        loads[name].start()

    barrier = pltpu.get_barrier_semaphore()
    for side in sides[:2]:
        pl.semaphore_signal(barrier, inc=1, device_id=side, device_id_type=MESH)
    for offset in range(1, N_LON):
        pl.semaphore_signal(
            barrier, inc=1, device_id={"lon": (lon + offset) % N_LON}, device_id_type=MESH
        )

    flow[BLOCKS] = jnp.zeros((FEATURES, ENTRIES), BF16)
    for owner in range(N_LON):
        for slot in range(CAP):
            index = out_source[owner * CAP + slot]
            filled = index < BLOCKS
            index = jnp.minimum(index, BLOCKS - 1)
            nodes = outflow_node[pl.ds(index, 1), :].astype(F32)
            pack_out[owner, pl.ds(slot, 1), :] = jnp.where(filled, nodes, -1.0)
            pack_out[owner, pl.ds(2 + slot, 1), :] = outflow_cell[pl.ds(index, 1), :].astype(F32)
            pack_out[owner, pl.ds(4 + slot, 1), :] = outflow_weight[pl.ds(index, 1), :]
        pack_out[owner, pl.ds(6, 2), :] = jnp.zeros((2, ENTRIES), F32)

    loads["fields"].wait()
    for j in range(ROWS):
        state_a[j] = tile[pl.ds(j, FEATURES, stride=ROWS), :]
    pl.semaphore_wait(barrier, N_LON + 1)

    east, north, mix = wind_east[...], wind_north[...], diffusion[...]
    c_west = jnp.maximum(east, 0.0) + mix
    c_east = mix - jnp.minimum(east, 0.0)
    c_south = jnp.maximum(north, 0.0) + mix
    c_north = mix - jnp.minimum(north, 0.0)
    c_middle = 1.0 - jnp.abs(east) - jnp.abs(north) - 4.0 * mix

    lane = lanes((GROUP, COLS))

    def send_edges(state, step):
        lat_out[step, 0] = state[0].astype(BF16)
        lat_out[step, 1] = state[ROWS - 1].astype(BF16)

        def collect(g, carry):
            for j in range(ROWS):
                part = state[j, pl.ds(pl.multiple_of(g * GROUP, GROUP), GROUP), :]
                moved = pltpu.roll(part, 16 * g + 2 * j + 1, 1)
                carry = jnp.where(lane // 2 == 8 * g + j, moved, carry)
            return carry

        edge = lax.fori_loop(0, GROUPS, collect, jnp.zeros((GROUP, COLS), F32))
        lon_out[step] = edge.astype(BF16)
        return [
            copy(lon_out.at[step], lon_in.at[step, 1], sides[2]),
            copy(lon_out.at[step], lon_in.at[step, 0], sides[3]),
            copy(lat_out.at[step, 0], lat_in.at[step, 1], sides[0]),
            copy(lat_out.at[step, 1], lat_in.at[step, 0], sides[1]),
        ]

    def advance(state, result, step, last):
        from_west = pltpu.roll(lon_in[step, 0].astype(F32), 1, 1)
        from_east = pltpu.roll(lon_in[step, 1].astype(F32), COLS - 1, 1)
        joined = jnp.where(lane % 2 == 0, from_east, from_west)

        def group(g, carry):
            at = pl.ds(pl.multiple_of(g * GROUP, GROUP), GROUP)
            low = jnp.where(lat == 0, state[0, at, :], lat_in[step, 0, at, :].astype(F32))
            high = jnp.where(
                lat == N_LAT - 1, state[ROWS - 1, at, :], lat_in[step, 1, at, :].astype(F32)
            )
            for j in range(ROWS):
                m = state[j, at, :]
                s = low if j == 0 else state[j - 1, at, :]
                n = high if j == ROWS - 1 else state[j + 1, at, :]
                ends = pltpu.roll(joined, 2 * COLS - (16 * g + 2 * j + 1), 1)
                w = jnp.where(lane == 0, ends, pltpu.roll(m, 1, 1))
                e = jnp.where(lane == COLS - 1, ends, pltpu.roll(m, COLS - 1, 1))
                row = slice(j, j + 1)
                value = m * c_middle[row] + w * c_west[row] + e * c_east[row]
                value = value + s * c_south[row] + n * c_north[row]
                result[j, at, :] = value
                if last:
                    grid_bf[at, j * COLS : (j + 1) * COLS] = value.astype(BF16)
            return carry

        lax.fori_loop(0, GROUPS, group, 0)

    first_edges = send_edges(state_a, 0)
    wanted = [
        copy(halo_rows, want_in.at[1], sides[0]),
        copy(halo_rows, want_in.at[0], sides[1]),
        copy(halo_rows, want_in.at[3], sides[2]),
        copy(halo_rows, want_in.at[2], sides[3]),
    ]
    packs = []
    for offset in range(1, N_LON):
        other = (lon + offset) % N_LON
        packs.append(copy(pack_out.at[other], pack_in.at[offset], {"lon": other}))
    pack_in[0] = pack_out[lon]

    def cell_table(k, carry):
        for half in range(2):
            cells = inflow_cell[pl.ds(2 * k + half, 1), :]
            for j in range(ROWS):
                cell_hot[k, j * COLS : (j + 1) * COLS, half * 128 : (half + 1) * 128] = hot(
                    sublanes((COLS, ENTRIES)) + j * COLS == cells
                )
        return carry

    lax.fori_loop(0, BLOCKS // 2, cell_table, 0)
    for c in first_edges:
        c.wait_recv()
    advance(state_a, state_b, 0, False)
    second_edges = send_edges(state_b, 1)

    def node_table(r, carry):
        node_hot[r] = hot(sublanes((NODES, ENTRIES)) == inflow_node[pl.ds(r, 1), :])
        return carry

    lax.fori_loop(0, BLOCKS, node_table, 0)
    node_hot[BLOCKS] = jnp.zeros((NODES, ENTRIES), BF16)
    for c in second_edges:
        c.wait_recv()
    advance(state_b, state_a, 1, True)

    def gather(k, carry):
        picked = mm(grid_bf[...], cell_hot[k])
        flow[2 * k] = (picked[:, :ENTRIES] * inflow_weight[pl.ds(2 * k, 1), :]).astype(BF16)
        flow[2 * k + 1] = (picked[:, ENTRIES:] * inflow_weight[pl.ds(2 * k + 1, 1), :]).astype(BF16)
        return carry

    lax.fori_loop(0, BLOCKS // 2, gather, 0)

    def share(dz, other, member):
        owner = 2 * ((z + dz + N_Z) % N_Z) + (1 - y if other else y)
        first, second = in_source[owner * CAP], in_source[owner * CAP + 1]
        rows = pl.ds(member * CHANNELS, CHANNELS)
        values = jnp.concatenate([flow[first, rows, :], flow[second, rows, :]], axis=1)
        places = jnp.concatenate([node_hot[first], node_hot[second]], axis=1)
        return nt_dot(values, places)

    order = (4, -3, 3, -2, 2, -1, 1, 0)
    hops = ((4, 3), (3, 4), (4, 3))
    y_copies, chains = {}, {}

    def send_y(k):
        rs_y_out[k] = share(order[k], True, 1).astype(BF16)
        y_copies[k] = copy(rs_y_out.at[k], rs_y_in.at[k], partner)

    def part(stream, dz):
        if stream < 2:
            return share(dz, stream == 0, 0)
        k = order.index(dz)
        y_copies[k].wait_recv()
        return share(dz, False, 1) + rs_y_in[k].astype(F32)

    def step_z(stream, s):
        for way in range(2):
            length = hops[stream][way]
            if s >= length:
                continue
            dz = (length - s) * (1 if way == 0 else -1)
            value = part(stream, dz)
            if s:
                chains[stream, way, s - 1].wait_recv()
                value = value + rs_in[stream, way, s - 1].astype(F32)
            rs_out[stream, way, s] = value.astype(BF16)
            chains[stream, way, s] = copy(
                rs_out.at[stream, way, s],
                rs_in.at[stream, way, s],
                above if way == 0 else below,
            )

    def end_z(stream):
        value = part(stream, 0)
        for way in range(2):
            last = hops[stream][way] - 1
            chains[stream, way, last].wait_recv()
            value = value + rs_in[stream, way, last].astype(F32)
        return value

    send_y(0)
    send_y(1)
    step_z(0, 0)
    step_z(1, 0)
    for k in range(2, 8):
        send_y(k)
    step_z(2, 0)

    def edge_table(k, carry):
        at = pl.ds(pl.multiple_of(k * 128, 128), 128)
        senders, receivers = edge_sender[pl.ds(k, 1), :], edge_receiver[pl.ds(k, 1), :]
        from_column, to_column = column(senders), column(receivers)
        for part_of in range(2):
            spot = lanes((128, 128)) + part_of * 128
            columns = slice(part_of * 128, part_of * 128 + 128)
            edge_hot[at, columns] = hot(from_column == spot)
            edge_hot[at, 256 + part_of * 128 : 384 + part_of * 128] = hot(to_column == spot)
            edge_hot[at, 512 + part_of * 128 : 640 + part_of * 128] = hot(
                from_column == spot + NODES
            )
            collect_hot[columns, at] = hot(sublanes((128, 128)) + part_of * 128 == receivers)
        return carry

    lax.fori_loop(0, EDGES // 128, edge_table, 0)
    for c in wanted:
        c.wait_recv()
    for q in range(4):
        rows = column(want_in[q, (q ^ 1) : (q ^ 1) + 1, :])[:HCAP]
        for part_of in range(2):
            want_hot[q, :, part_of * 128 : part_of * 128 + 128] = hot(
                rows == lanes((HCAP, 128)) + part_of * 128
            )
    for layer in range(LAYERS):
        halo[layer * NODES + 4 * HCAP : (layer + 1) * NODES, :] = jnp.zeros(
            (NODES - 4 * HCAP, MEMBERS * HID), BF16
        )

    for stream in range(3):
        step_z(stream, 1)
    for c in packs:
        c.wait_recv()

    def spread_table(k, carry):
        rows = pack_in[k]
        spot = sublanes((NODES, ENTRIES)).astype(F32)
        weights, places = [], []
        for slot in range(CAP):
            weights.append(
                jnp.where(spot == rows[slot : slot + 1], rows[4 + slot : 5 + slot], 0.0).astype(BF16)
            )
        weighted = jnp.concatenate(weights, axis=1)
        for j in range(4):
            places = [
                hot(spot + j * NODES == rows[2 + slot : 3 + slot]) for slot in range(CAP)
            ]
            spread[k, :, j * NODES : (j + 1) * NODES] = nt_dot(
                weighted, jnp.concatenate(places, axis=1)
            ).astype(BF16)
        return carry

    lax.fori_loop(0, 8, spread_table, 0)
    for stream in range(3):
        step_z(stream, 2)
    lax.fori_loop(8, 16, spread_table, 0)
    for stream in range(3):
        step_z(stream, 3)
    rs_last_out[...] = end_z(0).astype(BF16)
    last_y = copy(rs_last_out, rs_last_in, partner)
    near = end_z(1)
    node_input[CHANNELS:, :] = end_z(2)
    last_y.wait_recv()
    node_input[:CHANNELS, :] = near + rs_last_in[...].astype(F32)

    for name in ("encoder", "sender", "receiver", "update", "decoder"):
        loads[name].wait()
    turned = jnp.transpose(node_input[...]).astype(BF16)
    for m in range(MEMBERS):
        rows = pl.ds(m * NODES, NODES)
        hidden[rows, :] = silu(mm(turned[:, m * CHANNELS : (m + 1) * CHANNELS], encoder[...]))

    for layer in range(LAYERS):
        normed = normalize(hidden[...])
        source = mm(normed, sender_w[layer]).astype(BF16)
        source_target[:NODES, :HID] = source[:NODES]
        source_target[:NODES, HID:] = source[NODES:]
        travelling = []
        for q in range(4):
            halo_out[layer, q] = mm(want_hot[q], source_target[:NODES, :]).astype(BF16)
        for q in (2, 3, 0, 1):
            travelling.append(
                copy(halo_out.at[layer, q], halo_slot(halo, layer, q ^ 1), sides[q])
            )
        target = mm(normed, receiver_w[layer]).astype(BF16)
        source_target[NODES:, :HID] = target[:NODES]
        source_target[NODES:, HID:] = target[NODES:]

        def near_part(k, carry):
            at = pl.ds(pl.multiple_of(k * 256, 256), 256)
            summed[at, :] = mm(edge_hot[at, : 2 * NODES], source_target[...])
            return carry

        lax.fori_loop(0, EDGES // 256, near_part, 0)
        for c in travelling:
            c.wait_recv()
        base = layer * NODES

        def far_part(k, carry):
            at = pl.ds(pl.multiple_of(k * 256, 256), 256)
            value = summed[at, :] + mm(
                edge_hot[at, 2 * NODES :], halo[pl.ds(base, NODES), :]
            )
            message[at, :] = silu(value).astype(BF16)
            return carry

        lax.fori_loop(0, EDGES // 256, far_part, 0)
        collected = mm(collect_hot[...], message[...]).astype(BF16)
        for m in range(MEMBERS):
            rows = pl.ds(m * NODES, NODES)
            hidden[rows, :] += mm(collected[:, m * HID : (m + 1) * HID], update_w[layer])

    final = normalize(hidden[...])
    ring[0, 0] = nt_dot(decoder[...], final[:NODES]).astype(BF16)
    ring[2, 0] = nt_dot(decoder[...], final[NODES:]).astype(BF16)
    across = copy(ring.at[0, 0], ring.at[1, 0], partner)
    lengths = ((3, 4), (4, 3), (4, 3))
    moves, y_moves = {}, {}

    def slot_of(way, s):
        return s if way == 0 else (N_Z - s) % N_Z

    def forward(stream, s):
        for way in range(2):
            if s and s <= lengths[stream][way]:
                moves[stream, way, s - 1].wait_recv()
                if stream == 2:
                    here = slot_of(way, s)
                    y_moves[here] = copy(ring.at[2, here], ring_y.at[here], partner)
            if s < lengths[stream][way]:
                moves[stream, way, s] = copy(
                    ring.at[stream, slot_of(way, s)],
                    ring.at[stream, slot_of(way, s + 1)],
                    above if way == 0 else below,
                )

    def add(stream, slots, member):
        total = None
        for here in slots:
            if stream in (0, 2):
                k = (2 * here) % N_LON
            else:
                k = (2 * here + 2 * y + N_LON - 1) % N_LON
            values = ring_y[here] if stream == 3 else ring[stream, here]
            term = mm(values, spread[k])
            total = term if total is None else total + term
        adjust[member] += total

    def arrived(stream, s):
        if s == 0:
            return [0]
        return [slot_of(way, s) for way in range(2) if s <= lengths[stream][way]]

    forward(2, 0)
    forward(0, 0)
    y_moves[0] = copy(ring.at[2, 0], ring_y.at[0], partner)
    for m in range(MEMBERS):
        for j in range(ROWS):
            adjust[m, :, j * COLS : (j + 1) * COLS] = state_a[
                j, m * CHANNELS : (m + 1) * CHANNELS, :
            ]
    add(0, [0], 0)
    add(2, [0], 1)
    across.wait_recv()
    forward(1, 0)
    for s in range(1, 5):
        for stream in (2, 0, 1):
            forward(stream, s)
        add(1, arrived(1, s - 1), 0)
        for here in arrived(2, s - 1):
            y_moves[here].wait_recv()
        add(3, arrived(2, s - 1), 1)
        add(2, arrived(2, s), 1)
        add(0, arrived(0, s), 0)
    add(1, arrived(1, 4), 0)
    for here in arrived(2, 4):
        y_moves[here].wait_recv()
    add(3, arrived(2, 4), 1)

    for m in range(MEMBERS):
        for j in range(ROWS):
            tile[pl.ds(m * CHANNELS * ROWS + j, CHANNELS, stride=ROWS), :] = adjust[
                m, :, j * COLS : (j + 1) * COLS
            ]
    done = pltpu.make_async_copy(tile, out_hbm, load_sem.at[6])
    done.start()
    for c in started:
        c.wait_send()
    done.wait()


def halo_slot(halo, layer, q):
    return halo.at[pl.ds(layer * NODES + q * HCAP, HCAP), :]


def blocks_of(owners):
    owner = owners[:, 0]
    same = (owner[:, None] == owner[None, :]).astype(jnp.int32)
    earlier = jnp.sum(jnp.tril(same, -1), axis=1)
    slot = owner * CAP + earlier
    hits = slot[None, :] == jnp.arange(N_LON * CAP, dtype=jnp.int32)[:, None]
    return jnp.min(jnp.where(hits, jnp.arange(BLOCKS, dtype=jnp.int32)[None, :], BLOCKS), axis=1)


def body(
    fields,
    wind_east,
    wind_north,
    diffusion,
    inflow_owner,
    inflow_cell,
    inflow_node,
    inflow_weight,
    encoder,
    sender_weight,
    receiver_weight,
    update_weight,
    decoder,
    edge_sender,
    edge_receiver,
    halo_rows,
    outflow_owner,
    outflow_node,
    outflow_cell,
    outflow_weight,
):
    vmem = pl.BlockSpec(memory_space=pltpu.VMEM)
    smem = pl.BlockSpec(memory_space=pltpu.SMEM)
    anywhere = pl.BlockSpec(memory_space=pl.ANY)
    wanted = jnp.pad(halo_rows.reshape(4, HCAP), ((0, 4), (0, 128 - HCAP)))
    half = (CHANNELS, NODES)
    scratch = [
        pltpu.VMEM((FEATURES * ROWS, COLS), F32),
        pltpu.VMEM((ROWS, FEATURES, COLS), F32),
        pltpu.VMEM((ROWS, FEATURES, COLS), F32),
        pltpu.VMEM((2, 2, FEATURES, COLS), BF16),
        pltpu.VMEM((2, 2, FEATURES, COLS), BF16),
        pltpu.VMEM((2, GROUP, COLS), BF16),
        pltpu.VMEM((2, 2, GROUP, COLS), BF16),
        pltpu.VMEM((FEATURES, CELLS), BF16),
        pltpu.VMEM((BLOCKS // 2, CELLS, 2 * ENTRIES), BF16),
        pltpu.VMEM((BLOCKS + 1, FEATURES, ENTRIES), BF16),
        pltpu.VMEM((BLOCKS + 1, NODES, ENTRIES), BF16),
        pltpu.VMEM((N_LON, 8, ENTRIES), F32),
        pltpu.VMEM((N_LON, 8, ENTRIES), F32),
        pltpu.VMEM((4, 8, 128), jnp.int32),
        pltpu.VMEM((3, 2, 4) + half, BF16),
        pltpu.VMEM((3, 2, 4) + half, BF16),
        pltpu.VMEM((N_Z,) + half, BF16),
        pltpu.VMEM((N_Z,) + half, BF16),
        pltpu.VMEM(half, BF16),
        pltpu.VMEM(half, BF16),
        pltpu.VMEM((FEATURES, NODES), F32),
        pltpu.VMEM((EDGES, 3 * NODES), BF16),
        pltpu.VMEM((NODES, EDGES), BF16),
        pltpu.VMEM((4, HCAP, NODES), BF16),
        pltpu.VMEM((CHANNELS, HID), BF16),
        pltpu.VMEM((LAYERS, HID, HID), BF16),
        pltpu.VMEM((LAYERS, HID, HID), BF16),
        pltpu.VMEM((LAYERS, HID, HID), BF16),
        pltpu.VMEM((CHANNELS, HID), BF16),
        pltpu.VMEM((MEMBERS * NODES, HID), F32),
        pltpu.VMEM((2 * NODES, MEMBERS * HID), BF16),
        pltpu.VMEM((LAYERS, 4, HCAP, MEMBERS * HID), BF16),
        pltpu.VMEM((LAYERS * NODES, MEMBERS * HID), BF16),
        pltpu.VMEM((EDGES, MEMBERS * HID), F32),
        pltpu.VMEM((EDGES, MEMBERS * HID), BF16),
        pltpu.VMEM((N_LON, NODES, CELLS), BF16),
        pltpu.VMEM((3, N_Z) + half, BF16),
        pltpu.VMEM((N_Z,) + half, BF16),
        pltpu.VMEM((MEMBERS, CHANNELS, CELLS), F32),
        pltpu.SemaphoreType.DMA((8,)),
        pltpu.SemaphoreType.DMA((COPIES,)),
        pltpu.SemaphoreType.DMA((COPIES,)),
    ]
    result = pl.pallas_call(
        kernel,
        out_shape=jax.ShapeDtypeStruct((FEATURES * ROWS, COLS), F32),
        in_specs=[smem, smem, anywhere]
        + [vmem] * 6
        + [anywhere] * 5
        + [vmem] * 6,
        out_specs=anywhere,
        scratch_shapes=scratch,
        compiler_params=pltpu.CompilerParams(
            collective_id=0, has_side_effects=True, vmem_limit_bytes=VMEM_LIMIT
        ),
    )(
        blocks_of(inflow_owner),
        blocks_of(outflow_owner),
        fields.reshape(FEATURES * ROWS, COLS),
        wind_east,
        wind_north,
        diffusion,
        inflow_cell,
        inflow_node,
        inflow_weight,
        encoder,
        sender_weight,
        receiver_weight,
        update_weight,
        decoder.T,
        edge_sender.reshape(EDGES // 128, 128),
        edge_receiver.reshape(EDGES // 128, 128),
        wanted,
        outflow_node,
        outflow_cell,
        outflow_weight,
    )
    return result.reshape(MEMBERS, CHANNELS, ROWS, COLS)


def solution(mesh):
    placed = (
        P("member", None, "lat", "lon"),
        P("lat", "lon"),
        P("lat", "lon"),
        P("lat", "lon"),
        P(("lat", "lon"), None),
        P(("lat", "lon"), None),
        P(("lat", "lon"), None),
        P(("lat", "lon"), None),
        P(),
        P(),
        P(),
        P(),
        P(),
        P("lat", "lon", None),
        P("lat", "lon", None),
        P("lat", "lon", None, None),
        P(("lat", "lon"), None),
        P(("lat", "lon"), None),
        P(("lat", "lon"), None),
        P(("lat", "lon"), None),
    )
    return jax.shard_map(
        body, mesh=mesh, in_specs=placed, out_specs=P("member", None, "lat", "lon"), check_vma=False
    )
```

```python
import jax
import jax.numpy as jnp
from jax import lax
from jax.experimental import pallas as pl
from jax.experimental.pallas import tpu as pltpu
from jax.sharding import PartitionSpec as P

F32, BF16 = jnp.float32, jnp.bfloat16
MESH = pl.DeviceIdType.MESH
MEMBERS = 2
CHANNELS = 192
FEATURES = MEMBERS * CHANNELS
ROWS, COLS = 8, 128
CELLS = ROWS * COLS
BLOCKS, ENTRIES, CAP = 16, 128, 2
NODES = 256
HCAP = 48
EDGES = 1536
HID = 512
LAYERS = 2
DSTEPS = 2
N_LAT, N_LON = 8, 16
N_Z = N_LON // 2
GROUP = 48
GROUPS = CHANNELS // GROUP
HALF = CHANNELS // 2
COPIES = 192
VMEM_LIMIT = 63 * 1024 * 1024


def nt_dot(a, b):
    return lax.dot_general(a, b, (((1,), (1,)), ((), ())), preferred_element_type=F32)


def mm(a, b):
    return jnp.dot(a, b, preferred_element_type=F32)


def hot(mask):
    return jnp.where(mask, 1.0, 0.0).astype(BF16)


def silu(v):
    half = 0.5 * v
    return half + half * jnp.tanh(half)


def normalize(values):
    scale = lax.rsqrt(jnp.mean(values * values, axis=-1, keepdims=True) + 1e-06)
    return (values * scale).astype(BF16)


def lanes(shape):
    return lax.broadcasted_iota(jnp.int32, shape, 1)


def sublanes(shape):
    return lax.broadcasted_iota(jnp.int32, shape, 0)


def column(row):
    return jnp.transpose(jnp.broadcast_to(row.astype(F32), (128, 128))).astype(jnp.int32)


def kernel(
    inflow_owner,
    outflow_owner,
    fields_hbm,
    wind_east,
    wind_north,
    diffusion,
    inflow_cell,
    inflow_node,
    inflow_weight,
    encoder_hbm,
    sender_hbm,
    receiver_hbm,
    update_hbm,
    decoder_hbm,
    edge_sender,
    edge_receiver,
    halo_rows,
    outflow_node,
    outflow_cell,
    outflow_weight,
    out_hbm,
    tile,
    state_a,
    state_b,
    lat_out,
    lat_in,
    lon_out,
    lon_in,
    grid_bf,
    cell_hot,
    flow,
    node_hot,
    pack_out,
    pack_in,
    want_in,
    shares,
    rs_out,
    rs_in,
    rs_y_out,
    rs_y_in,
    rs_last_out,
    rs_last_in,
    node_input,
    edge_hot,
    collect_hot,
    want_hot,
    encoder,
    sender_w,
    receiver_w,
    update_w,
    decoder,
    hidden,
    source_target,
    halo_out,
    halo,
    summed,
    message,
    spread,
    both,
    adjust,
    in_source,
    want_out,
    load_sem,
    send_sem,
    recv_sem,
):
    lat = lax.axis_index("lat")
    lon = lax.axis_index("lon")
    z, y = lon // 2, lon % 2
    sides = (
        {"lat": (lat + N_LAT - 1) % N_LAT},
        {"lat": (lat + 1) % N_LAT},
        {"lon": (lon + N_LON - 1) % N_LON},
        {"lon": (lon + 1) % N_LON},
    )
    above = {"lon": (lon + 2) % N_LON}
    below = {"lon": (lon + N_LON - 2) % N_LON}
    partner = {"lon": 2 * z + (1 - y)}
    used = [0]
    started = []

    def copy(src, dst, device):
        index = used[0]
        used[0] += 1
        made = pltpu.make_async_remote_copy(
            src_ref=src,
            dst_ref=dst,
            send_sem=send_sem.at[index],
            recv_sem=recv_sem.at[index],
            device_id=device,
            device_id_type=MESH,
        )
        made.start()
        started.append(made)
        return made

    loads = {}
    for index, (name, src, dst) in enumerate(
        (
            ("fields0", fields_hbm.at[0], tile.at[0]),
            ("fields1", fields_hbm.at[1], tile.at[1]),
            ("encoder", encoder_hbm, encoder),
            ("sender", sender_hbm, sender_w),
            ("receiver", receiver_hbm, receiver_w),
            ("update", update_hbm, update_w),
            ("decoder", decoder_hbm, decoder),
        )
    ):
        loads[name] = pltpu.make_async_copy(src, dst, load_sem.at[index])
        loads[name].start()

    barrier = pltpu.get_barrier_semaphore()
    for side in sides[:2]:
        pl.semaphore_signal(barrier, inc=1, device_id=side, device_id_type=MESH)
    for offset in range(1, N_LON):
        pl.semaphore_signal(
            barrier, inc=1, device_id={"lon": (lon + offset) % N_LON}, device_id_type=MESH
        )

    def blocks_of(owners, owner):
        first, second = jnp.int32(BLOCKS), jnp.int32(BLOCKS)
        for r in reversed(range(BLOCKS)):
            same = owners[0, r] == owner
            second = jnp.where(same, first, second)
            first = jnp.where(same, r, first)
        return first, second

    for owner in range(N_LON):
        pair = blocks_of(inflow_owner, owner)
        for slot in range(CAP):
            in_source[owner * CAP + slot] = pair[slot]
    want_out[...] = jnp.zeros((8, 128), jnp.int32)
    want_out[:4, :HCAP] = halo_rows[0, 0]

    flow[BLOCKS] = jnp.zeros((FEATURES, ENTRIES), BF16)
    for owner in range(N_LON):
        pair = blocks_of(outflow_owner, owner)
        for slot in range(CAP):
            index = pair[slot]
            filled = index < BLOCKS
            index = jnp.minimum(index, BLOCKS - 1)
            nodes = outflow_node[pl.ds(index, 1), :].astype(F32)
            pack_out[owner, pl.ds(slot, 1), :] = jnp.where(filled, nodes, -1.0)
            pack_out[owner, pl.ds(2 + slot, 1), :] = outflow_cell[pl.ds(index, 1), :].astype(F32)
            pack_out[owner, pl.ds(4 + slot, 1), :] = outflow_weight[pl.ds(index, 1), :]
        pack_out[owner, pl.ds(6, 2), :] = jnp.zeros((2, ENTRIES), F32)

    for m in range(MEMBERS):
        loads[f"fields{m}"].wait()
        for j in range(ROWS):
            state_a[j, m * CHANNELS : (m + 1) * CHANNELS, :] = tile[
                m, pl.ds(j, CHANNELS, stride=ROWS), :
            ]
    pl.semaphore_wait(barrier, N_LON + 1)

    east, north, mix = wind_east[...], wind_north[...], diffusion[...]
    c_west = jnp.maximum(east, 0.0) + mix
    c_east = mix - jnp.minimum(east, 0.0)
    c_south = jnp.maximum(north, 0.0) + mix
    c_north = mix - jnp.minimum(north, 0.0)
    c_middle = 1.0 - jnp.abs(east) - jnp.abs(north) - 4.0 * mix

    lane = lanes((GROUP, COLS))

    def send_edges(state, step, m):
        rows = slice(m * CHANNELS, (m + 1) * CHANNELS)
        lat_out[step, m, 0] = state[0, rows].astype(BF16)
        lat_out[step, m, 1] = state[ROWS - 1, rows].astype(BF16)

        def collect(g, carry):
            at = pl.ds(pl.multiple_of(m * CHANNELS + g * GROUP, GROUP), GROUP)
            for j in range(ROWS):
                moved = pltpu.roll(state[j, at, :], 16 * g + 2 * j + 1, 1)
                carry = jnp.where(lane // 2 == 8 * g + j, moved, carry)
            return carry

        edge = lax.fori_loop(0, GROUPS, collect, jnp.zeros((GROUP, COLS), F32))
        lon_out[step, m] = edge.astype(BF16)
        return [
            copy(lon_out.at[step, m], lon_in.at[step, m, 1], sides[2]),
            copy(lon_out.at[step, m], lon_in.at[step, m, 0], sides[3]),
            copy(lat_out.at[step, m, 0], lat_in.at[step, m, 1], sides[0]),
            copy(lat_out.at[step, m, 1], lat_in.at[step, m, 0], sides[1]),
        ]

    def advance(state, result, step, m, last):
        from_west = pltpu.roll(lon_in[step, m, 0].astype(F32), 1, 1)
        from_east = pltpu.roll(lon_in[step, m, 1].astype(F32), COLS - 1, 1)
        joined = jnp.where(lane % 2 == 0, from_east, from_west)

        def group(g, carry):
            inner = pl.ds(pl.multiple_of(g * GROUP, GROUP), GROUP)
            at = pl.ds(pl.multiple_of(m * CHANNELS + g * GROUP, GROUP), GROUP)
            low = jnp.where(lat == 0, state[0, at, :], lat_in[step, m, 0, inner, :].astype(F32))
            high = jnp.where(
                lat == N_LAT - 1,
                state[ROWS - 1, at, :],
                lat_in[step, m, 1, inner, :].astype(F32),
            )
            for j in range(ROWS):
                center = state[j, at, :]
                s = low if j == 0 else state[j - 1, at, :]
                n = high if j == ROWS - 1 else state[j + 1, at, :]
                ends = pltpu.roll(joined, 2 * COLS - (16 * g + 2 * j + 1), 1)
                w = jnp.where(lane == 0, ends, pltpu.roll(center, 1, 1))
                e = jnp.where(lane == COLS - 1, ends, pltpu.roll(center, COLS - 1, 1))
                row = slice(j, j + 1)
                value = center * c_middle[row] + w * c_west[row] + e * c_east[row]
                value = value + s * c_south[row] + n * c_north[row]
                result[j, at, :] = value
                if last:
                    grid_bf[at, j * COLS : (j + 1) * COLS] = value.astype(BF16)
            return carry

        lax.fori_loop(0, GROUPS, group, 0)

    def arrive(copies):
        for c in copies:
            c.wait_recv()

    first = [send_edges(state_a, 0, m) for m in range(MEMBERS)]
    wanted = [
        copy(want_out, want_in.at[1], sides[0]),
        copy(want_out, want_in.at[0], sides[1]),
        copy(want_out, want_in.at[3], sides[2]),
        copy(want_out, want_in.at[2], sides[3]),
    ]
    packs = []
    for offset in range(1, N_LON):
        other = (lon + offset) % N_LON
        packs.append(copy(pack_out.at[other], pack_in.at[offset], {"lon": other}))
    pack_in[0] = pack_out[lon]

    def cell_table(k, carry):
        for half in range(2):
            cells = inflow_cell[pl.ds(2 * k + half, 1), :]
            for j in range(ROWS):
                cell_hot[k, j * COLS : (j + 1) * COLS, half * 128 : (half + 1) * 128] = hot(
                    sublanes((COLS, ENTRIES)) + j * COLS == cells
                )
        return carry

    lax.fori_loop(0, BLOCKS // 2, cell_table, 0)
    def edge_table(k, carry):
        at = pl.ds(pl.multiple_of(k * 128, 128), 128)
        senders, receivers = edge_sender[0, :, at], edge_receiver[0, :, at]
        from_column, to_column = column(senders), column(receivers)
        for part_of in range(2):
            spot = lanes((128, 128)) + part_of * 128
            columns = slice(part_of * 128, part_of * 128 + 128)
            edge_hot[at, columns] = hot(from_column == spot)
            edge_hot[at, 256 + part_of * 128 : 384 + part_of * 128] = hot(to_column == spot)
            edge_hot[at, 512 + part_of * 128 : 640 + part_of * 128] = hot(
                from_column == spot + NODES
            )
            collect_hot[columns, at] = hot(sublanes((128, 128)) + part_of * 128 == receivers)
        return carry

    lax.fori_loop(0, EDGES // 128, edge_table, 0)
    second = []
    for m in range(MEMBERS):
        arrive(first[m])
        advance(state_a, state_b, 0, m, False)
        second.append(send_edges(state_b, 1, m))

    def node_table(r, carry):
        node_hot[r] = hot(sublanes((NODES, ENTRIES)) == inflow_node[pl.ds(r, 1), :])
        return carry

    lax.fori_loop(0, BLOCKS, node_table, 0)
    node_hot[BLOCKS] = jnp.zeros((NODES, ENTRIES), BF16)

    def gather(k, carry):
        picked = mm(grid_bf[...], cell_hot[k])
        for half in range(2):
            weights = inflow_weight[pl.ds(2 * k + half, 1), :]
            flow[2 * k + half] = (
                picked[:, half * ENTRIES : (half + 1) * ENTRIES] * weights
            ).astype(BF16)
        return carry

    known = set()

    def share(m, dz, other, rows):
        spot = 2 * (dz % N_Z) + (1 if other else 0)
        if spot not in known:
            known.add(spot)
            owner = 2 * ((z + dz + N_Z) % N_Z) + (1 - y if other else y)
            one, two = in_source[owner * CAP], in_source[owner * CAP + 1]
            values = jnp.concatenate([flow[one], flow[two]], axis=1)
            places = jnp.concatenate([node_hot[one], node_hot[two]], axis=1)
            shares[spot] = nt_dot(values, places)
        return shares[spot, m * CHANNELS + rows.start : m * CHANNELS + rows.stop]

    order = (4, -3, 3, -2, 2, -1, 1, 0)
    hops = ((4, 3), (3, 4), (4, 3))
    lower, upper = slice(0, HALF), slice(HALF, CHANNELS)

    def reduce_scatter(m):
        y_copies, chains = {}, {}

        def send_y(k):
            rs_y_out[m, k] = share(m, order[k], True, upper).astype(BF16)
            y_copies[k] = copy(rs_y_out.at[m, k], rs_y_in.at[m, k], partner)

        def part(stream, dz):
            if stream < 2:
                return share(m, dz, stream == 0, lower)
            k = order.index(dz)
            y_copies[k].wait_recv()
            return share(m, dz, False, upper) + rs_y_in[m, k].astype(F32)

        def step_z(stream, s):
            for way in range(2):
                length = hops[stream][way]
                if s >= length:
                    continue
                dz = (length - s) * (1 if way == 0 else -1)
                value = part(stream, dz)
                if s:
                    chains[stream, way, s - 1].wait_recv()
                    value = value + rs_in[m, stream, way, s - 1].astype(F32)
                rs_out[m, stream, way, s] = value.astype(BF16)
                chains[stream, way, s] = copy(
                    rs_out.at[m, stream, way, s],
                    rs_in.at[m, stream, way, s],
                    above if way == 0 else below,
                )

        def end_z(stream):
            value = part(stream, 0)
            for way in range(2):
                last = hops[stream][way] - 1
                chains[stream, way, last].wait_recv()
                value = value + rs_in[m, stream, way, last].astype(F32)
            return value

        def begin():
            send_y(0)
            send_y(1)
            step_z(0, 0)
            step_z(1, 0)

        def rest_y():
            for k in range(2, 8):
                send_y(k)

        last_y = []

        def end_first():
            rs_last_out[m] = end_z(0).astype(BF16)
            last_y.append(copy(rs_last_out.at[m], rs_last_in.at[m], partner))

        def end_others():
            node_input[m, lower] = end_z(1)
            node_input[m, upper] = end_z(2)

        def end():
            arrive(last_y)
            node_input[m, lower] += rs_last_in[m].astype(F32)

        return begin, rest_y, step_z, end_first, end_others, end

    def run(work, count=1):
        for _ in range(count):
            next(work, None)

    def finish(work):
        for _ in work:
            pass

    def network(m):
        turned = jnp.transpose(
            jnp.concatenate([node_input[m], jnp.zeros((64, NODES), F32)], axis=0)
        )[:, :CHANNELS].astype(BF16)
        hidden[m] = silu(mm(turned, encoder[...]))
        yield
        for layer in range(LAYERS):
            normed = normalize(hidden[m])
            source_target[m, :NODES] = mm(normed, sender_w[layer]).astype(BF16)
            travelling = []
            for q in (2, 3, 0, 1):
                halo_out[m, layer, q] = mm(want_hot[q], source_target[m, :NODES]).astype(BF16)
                travelling.append(
                    copy(
                        halo_out.at[m, layer, q],
                        halo.at[m, layer, pl.ds((q ^ 1) * HCAP, HCAP)],
                        sides[q],
                    )
                )
            yield
            source_target[m, NODES:] = mm(normed, receiver_w[layer]).astype(BF16)
            for k in range(3):
                at = slice(k * 512, (k + 1) * 512)
                summed[m, at] = mm(edge_hot[at, : 2 * NODES], source_target[m])
                yield
            arrive(travelling)
            for k in range(3):
                at = slice(k * 512, (k + 1) * 512)
                value = summed[m, at] + mm(edge_hot[at, 2 * NODES :], halo[m, layer])
                message[m, at] = silu(value).astype(BF16)
                yield
            collected = mm(collect_hot[...], message[m]).astype(BF16)
            hidden[m] += mm(collected, update_w[layer])
            yield
        both[m, 0, 0] = nt_dot(decoder[...], normalize(hidden[m])).astype(BF16)

    lengths = ((3, 4), (4, 3), (4, 3))
    low_half, high_half = pl.ds(0, HALF), pl.ds(HALF, HALF)

    def slot_of(way, s):
        return s if way == 0 else (N_Z - s) % N_Z

    def gather_all(m):
        moves, y_moves = {}, {}

        def view(stream, slot):
            return both.at[m, stream % 2, slot, high_half if stream == 2 else low_half]

        def pass_y(slot):
            y_moves[slot] = copy(
                both.at[m, 0, slot, high_half], both.at[m, 1, slot, high_half], partner
            )

        def forward(stream, s):
            for way in range(2):
                if s and s <= lengths[stream][way]:
                    moves[stream, way, s - 1].wait_recv()
                    if stream == 2:
                        pass_y(slot_of(way, s))
                if s < lengths[stream][way]:
                    moves[stream, way, s] = copy(
                        view(stream, slot_of(way, s)),
                        view(stream, slot_of(way, s + 1)),
                        above if way == 0 else below,
                    )

        def add(side, slots):
            total = None
            for slot in slots:
                if side:
                    y_moves[slot].wait_recv()
                    k = (2 * slot + 2 * y + N_LON - 1) % N_LON
                else:
                    k = 2 * slot
                term = mm(both[m, side, slot], spread[k])
                total = term if total is None else total + term
            adjust[m] += total

        across = []

        def begin():
            across.append(copy(view(0, 0), view(1, 0), partner))
            forward(2, 0)
            forward(0, 0)
            pass_y(0)

        def begin_other():
            arrive(across)
            forward(1, 0)

        def end():
            for j in range(ROWS):
                tile[m, pl.ds(j, CHANNELS, stride=ROWS), :] = adjust[
                    m, :, j * COLS : (j + 1) * COLS
                ]
            done = pltpu.make_async_copy(tile.at[m], out_hbm.at[m], load_sem.at[7 + m])
            done.start()
            results.append(done)

        return begin, begin_other, forward, add, end

    results = []

    def wanted_table():
        arrive(wanted)
        for q in range(4):
            rows = column(want_in[q, (q ^ 1) : (q ^ 1) + 1, :])[:HCAP]
            for part_of in range(2):
                want_hot[q, :, part_of * 128 : part_of * 128 + 128] = hot(
                    rows == lanes((HCAP, 128)) + part_of * 128
                )
        for m in range(MEMBERS):
            for layer in range(LAYERS):
                halo[m, layer, 4 * HCAP :] = jnp.zeros((NODES - 4 * HCAP, HID), BF16)

    def spread_table(k, carry):
        rows = pack_in[k]
        spot = sublanes((NODES, ENTRIES)).astype(F32)
        weights, places = [], []
        for slot in range(CAP):
            weights.append(
                jnp.where(spot == rows[slot : slot + 1], rows[4 + slot : 5 + slot], 0.0).astype(BF16)
            )
        weighted = jnp.concatenate(weights, axis=1)
        for j in range(4):
            places = [
                hot(spot + j * NODES == rows[2 + slot : 3 + slot]) for slot in range(CAP)
            ]
            spread[k, :, j * NODES : (j + 1) * NODES] = nt_dot(
                weighted, jnp.concatenate(places, axis=1)
            ).astype(BF16)
        return carry

    arrive(packs)
    wanted_table()
    lax.fori_loop(0, 4, spread_table, 0)
    arrive(second[0])
    arrive(second[1])
    for m in range(MEMBERS):
        advance(state_b, state_a, 1, m, True)
    lax.fori_loop(0, BLOCKS // 2, gather, 0)
    sums = [reduce_scatter(m) for m in range(MEMBERS)]
    begin0, rest0, step0, first0, others0, end0 = sums[0]
    begin1, rest1, step1, first1, others1, end1 = sums[1]
    begin0()
    begin1()
    rest0()
    lax.fori_loop(4, 8, spread_table, 0)
    step0(2, 0)
    rest1()
    step0(0, 1)
    step0(1, 1)
    step1(0, 1)
    step1(1, 1)
    step1(2, 0)
    lax.fori_loop(8, 12, spread_table, 0)
    step0(2, 1)
    step0(0, 2)
    step0(1, 2)
    step1(0, 2)
    step1(1, 2)
    lax.fori_loop(12, 16, spread_table, 0)
    step0(2, 2)
    step0(0, 3)
    step0(1, 3)
    step1(2, 1)
    step1(0, 3)
    step1(1, 3)
    for name in ("encoder", "sender", "receiver", "update", "decoder"):
        loads[name].wait()
    step0(2, 3)
    first0()
    step1(2, 2)
    first1()
    others0()
    end0()
    nets = [network(m) for m in range(MEMBERS)]
    net0, net1 = nets
    start_a, other_a, pass_a, add_a, end_a = gather_all(0)
    start_b, other_b, pass_b, add_b, end_b = gather_all(1)
    run(net0, 2)
    step1(2, 3)
    run(net0, 3)
    others1()
    end1()
    run(net1, 2)
    run(net1, 3)
    run(net0)
    run(net0, 4)
    run(net1)
    run(net1, 4)
    run(net0, 3)
    run(net0)
    finish(net0)
    start_a()
    for m in range(MEMBERS):
        for j in range(ROWS):
            adjust[m, :, j * COLS : (j + 1) * COLS] = state_a[
                j, m * CHANNELS : (m + 1) * CHANNELS, :
            ]
    run(net1, 3)
    run(net1)
    finish(net1)
    start_b()
    other_a()
    pass_a(2, 1)
    pass_a(0, 1)
    add_a(0, [0])
    add_b(0, [0])
    other_b()
    pass_b(2, 1)
    pass_b(0, 1)
    pass_a(2, 2)
    pass_a(1, 1)
    pass_a(0, 2)
    add_a(1, [0])
    pass_b(2, 2)
    pass_b(1, 1)
    pass_b(0, 2)
    add_a(0, [1, 7])
    add_b(1, [0])
    pass_a(2, 3)
    pass_a(1, 2)
    pass_a(0, 3)
    add_a(1, [1, 7])
    add_b(0, [1, 7])
    pass_b(2, 3)
    pass_b(1, 2)
    pass_b(0, 3)
    add_b(1, [1, 7])
    add_a(0, [2, 6])
    pass_a(2, 4)
    pass_a(1, 3)
    pass_a(0, 4)
    add_a(1, [2, 6])
    add_a(0, [3, 5])
    add_a(0, [4])
    add_b(0, [2, 6])
    pass_b(2, 4)
    pass_b(1, 3)
    pass_b(0, 4)
    add_b(1, [2, 6])
    add_b(0, [3, 5])
    add_b(0, [4])
    pass_a(1, 4)
    add_a(1, [3, 5])
    add_a(1, [4])
    end_a()
    pass_b(1, 4)
    add_b(1, [3, 5])
    add_b(1, [4])
    end_b()
    for c in started:
        c.wait_send()
    for c in results:
        c.wait()


def body(
    fields,
    wind_east,
    wind_north,
    diffusion,
    inflow_owner,
    inflow_cell,
    inflow_node,
    inflow_weight,
    encoder,
    sender_weight,
    receiver_weight,
    update_weight,
    decoder,
    edge_sender,
    edge_receiver,
    halo_rows,
    outflow_owner,
    outflow_node,
    outflow_cell,
    outflow_weight,
):
    vmem = pl.BlockSpec(memory_space=pltpu.VMEM)
    smem = pl.BlockSpec(memory_space=pltpu.SMEM)
    anywhere = pl.BlockSpec(memory_space=pl.ANY)
    half = (HALF, NODES)
    scratch = [
        pltpu.VMEM((MEMBERS, CHANNELS * ROWS, COLS), F32),
        pltpu.VMEM((ROWS, FEATURES, COLS), F32),
        pltpu.VMEM((ROWS, FEATURES, COLS), F32),
        pltpu.VMEM((DSTEPS, MEMBERS, 2, CHANNELS, COLS), BF16),
        pltpu.VMEM((DSTEPS, MEMBERS, 2, CHANNELS, COLS), BF16),
        pltpu.VMEM((DSTEPS, MEMBERS, GROUP, COLS), BF16),
        pltpu.VMEM((DSTEPS, MEMBERS, 2, GROUP, COLS), BF16),
        pltpu.VMEM((FEATURES, CELLS), BF16),
        pltpu.VMEM((BLOCKS // 2, CELLS, 2 * ENTRIES), BF16),
        pltpu.VMEM((BLOCKS + 1, FEATURES, ENTRIES), BF16),
        pltpu.VMEM((BLOCKS + 1, NODES, ENTRIES), BF16),
        pltpu.VMEM((N_LON, 8, ENTRIES), F32),
        pltpu.VMEM((N_LON, 8, ENTRIES), F32),
        pltpu.VMEM((4, 8, 128), jnp.int32),
        pltpu.VMEM((N_LON, FEATURES, NODES), F32),
        pltpu.VMEM((MEMBERS, 3, 2, 4) + half, BF16),
        pltpu.VMEM((MEMBERS, 3, 2, 4) + half, BF16),
        pltpu.VMEM((MEMBERS, N_Z) + half, BF16),
        pltpu.VMEM((MEMBERS, N_Z) + half, BF16),
        pltpu.VMEM((MEMBERS,) + half, BF16),
        pltpu.VMEM((MEMBERS,) + half, BF16),
        pltpu.VMEM((MEMBERS, CHANNELS, NODES), F32),
        pltpu.VMEM((EDGES, 3 * NODES), BF16),
        pltpu.VMEM((NODES, EDGES), BF16),
        pltpu.VMEM((4, HCAP, NODES), BF16),
        pltpu.VMEM((CHANNELS, HID), BF16),
        pltpu.VMEM((LAYERS, HID, HID), BF16),
        pltpu.VMEM((LAYERS, HID, HID), BF16),
        pltpu.VMEM((LAYERS, HID, HID), BF16),
        pltpu.VMEM((CHANNELS, HID), BF16),
        pltpu.VMEM((MEMBERS, NODES, HID), F32),
        pltpu.VMEM((MEMBERS, 2 * NODES, HID), BF16),
        pltpu.VMEM((MEMBERS, LAYERS, 4, HCAP, HID), BF16),
        pltpu.VMEM((MEMBERS, LAYERS, NODES, HID), BF16),
        pltpu.VMEM((MEMBERS, EDGES, HID), F32),
        pltpu.VMEM((MEMBERS, EDGES, HID), BF16),
        pltpu.VMEM((N_LON, NODES, CELLS), BF16),
        pltpu.VMEM((MEMBERS, 2, N_Z, CHANNELS, NODES), BF16),
        pltpu.VMEM((MEMBERS, CHANNELS, CELLS), F32),
        pltpu.SMEM((N_LON * CAP,), jnp.int32),
        pltpu.VMEM((8, 128), jnp.int32),
        pltpu.SemaphoreType.DMA((9,)),
        pltpu.SemaphoreType.DMA((COPIES,)),
        pltpu.SemaphoreType.DMA((COPIES,)),
    ]
    result = pl.pallas_call(
        kernel,
        out_shape=jax.ShapeDtypeStruct((MEMBERS, CHANNELS * ROWS, COLS), F32),
        in_specs=[smem, smem, anywhere]
        + [vmem] * 6
        + [anywhere] * 5
        + [vmem] * 6,
        out_specs=anywhere,
        scratch_shapes=scratch,
        compiler_params=pltpu.CompilerParams(
            collective_id=0, has_side_effects=True, vmem_limit_bytes=VMEM_LIMIT
        ),
    )(
        inflow_owner.reshape(1, BLOCKS),
        outflow_owner.reshape(1, BLOCKS),
        fields.reshape(MEMBERS, CHANNELS * ROWS, COLS),
        wind_east,
        wind_north,
        diffusion,
        inflow_cell,
        inflow_node,
        inflow_weight,
        encoder,
        sender_weight,
        receiver_weight,
        update_weight,
        decoder.T,
        edge_sender,
        edge_receiver,
        halo_rows,
        outflow_node,
        outflow_cell,
        outflow_weight,
    )
    return result.reshape(MEMBERS, CHANNELS, ROWS, COLS)


def solution(mesh):
    placed = (
        P("member", None, "lat", "lon"),
        P("lat", "lon"),
        P("lat", "lon"),
        P("lat", "lon"),
        P(("lat", "lon"), None),
        P(("lat", "lon"), None),
        P(("lat", "lon"), None),
        P(("lat", "lon"), None),
        P(),
        P(),
        P(),
        P(),
        P(),
        P("lat", "lon", None),
        P("lat", "lon", None),
        P("lat", "lon", None, None),
        P(("lat", "lon"), None),
        P(("lat", "lon"), None),
        P(("lat", "lon"), None),
        P(("lat", "lon"), None),
    )
    return jax.shard_map(
        body, mesh=mesh, in_specs=placed, out_specs=P("member", None, "lat", "lon"), check_vma=False
    )
```

```python
import jax
import jax.numpy as jnp
from jax import lax
from jax.experimental import pallas as pl
from jax.experimental.pallas import tpu as pltpu
from jax.sharding import PartitionSpec as P

F32, BF16 = jnp.float32, jnp.bfloat16
MESH = pl.DeviceIdType.MESH
MEMBERS = 2
CHANNELS = 192
FEATURES = MEMBERS * CHANNELS
ROWS, COLS = 8, 128
CELLS = ROWS * COLS
BLOCKS, ENTRIES, CAP = 16, 128, 2
NODES = 256
HCAP = 48
EDGES = 1536
HID = 512
LAYERS = 2
DSTEPS = 2
N_LAT, N_LON = 8, 16
N_Z = N_LON // 2
GROUP = 48
GROUPS = CHANNELS // GROUP
HALF = 80
COPIES = 192
VMEM_LIMIT = 63 * 1024 * 1024


def nt_dot(a, b):
    return lax.dot_general(a, b, (((1,), (1,)), ((), ())), preferred_element_type=F32)


def mm(a, b):
    return jnp.dot(a, b, preferred_element_type=F32)


def hot(mask):
    return jnp.where(mask, 1.0, 0.0).astype(BF16)


def silu(v):
    half = 0.5 * v
    return half + half * jnp.tanh(half)


def normalize(values):
    scale = lax.rsqrt(jnp.mean(values * values, axis=-1, keepdims=True) + 1e-06)
    return (values * scale).astype(BF16)


def lanes(shape):
    return lax.broadcasted_iota(jnp.int32, shape, 1)


def sublanes(shape):
    return lax.broadcasted_iota(jnp.int32, shape, 0)


def column(row):
    return jnp.transpose(jnp.broadcast_to(row.astype(F32), (128, 128))).astype(jnp.int32)


def kernel(
    inflow_owner,
    outflow_owner,
    fields_hbm,
    wind_east,
    wind_north,
    diffusion,
    inflow_cell,
    inflow_node,
    inflow_weight,
    encoder_hbm,
    sender_hbm,
    receiver_hbm,
    update_hbm,
    decoder_hbm,
    edge_sender,
    edge_receiver,
    halo_rows,
    outflow_node,
    outflow_cell,
    outflow_weight,
    out_hbm,
    tile,
    state_a,
    state_b,
    lat_out,
    lat_in,
    lon_out,
    lon_in,
    grid_bf,
    cell_hot,
    flow,
    node_hot,
    pack_out,
    pack_in,
    want_in,
    shares,
    rs_out,
    rs_in,
    rs_y_out,
    rs_y_in,
    rs_last_out,
    rs_last_in,
    node_input,
    edge_hot,
    collect_hot,
    want_hot,
    encoder,
    sender_w,
    receiver_w,
    update_w,
    decoder,
    hidden,
    source_target,
    halo_out,
    halo,
    summed,
    message,
    spread,
    both,
    adjust,
    in_source,
    want_out,
    load_sem,
    send_sem,
    recv_sem,
):
    lat = lax.axis_index("lat")
    lon = lax.axis_index("lon")
    z, y = lon // 2, lon % 2
    sides = (
        {"lat": (lat + N_LAT - 1) % N_LAT},
        {"lat": (lat + 1) % N_LAT},
        {"lon": (lon + N_LON - 1) % N_LON},
        {"lon": (lon + 1) % N_LON},
    )
    above = {"lon": (lon + 2) % N_LON}
    below = {"lon": (lon + N_LON - 2) % N_LON}
    partner = {"lon": 2 * z + (1 - y)}
    used = [0]
    started = []

    def copy(src, dst, device):
        index = used[0]
        used[0] += 1
        made = pltpu.make_async_remote_copy(
            src_ref=src,
            dst_ref=dst,
            send_sem=send_sem.at[index],
            recv_sem=recv_sem.at[index],
            device_id=device,
            device_id_type=MESH,
        )
        made.start()
        started.append(made)
        return made

    loads = {}
    for index, (name, src, dst) in enumerate(
        (
            ("fields0", fields_hbm.at[0], tile.at[0]),
            ("fields1", fields_hbm.at[1], tile.at[1]),
            ("encoder", encoder_hbm, encoder),
            ("sender", sender_hbm, sender_w),
            ("receiver", receiver_hbm, receiver_w),
            ("update", update_hbm, update_w),
            ("decoder", decoder_hbm, decoder),
        )
    ):
        loads[name] = pltpu.make_async_copy(src, dst, load_sem.at[index])
        loads[name].start()

    barrier = pltpu.get_barrier_semaphore()
    for side in sides[:2]:
        pl.semaphore_signal(barrier, inc=1, device_id=side, device_id_type=MESH)
    for offset in range(1, N_LON):
        pl.semaphore_signal(
            barrier, inc=1, device_id={"lon": (lon + offset) % N_LON}, device_id_type=MESH
        )

    def blocks_of(owners, owner):
        first, second = jnp.int32(BLOCKS), jnp.int32(BLOCKS)
        for r in reversed(range(BLOCKS)):
            same = owners[0, r] == owner
            second = jnp.where(same, first, second)
            first = jnp.where(same, r, first)
        return first, second

    for owner in range(N_LON):
        pair = blocks_of(inflow_owner, owner)
        for slot in range(CAP):
            in_source[owner * CAP + slot] = pair[slot]
    want_out[...] = jnp.zeros((8, 128), jnp.int32)
    want_out[:4, :HCAP] = halo_rows[0, 0]

    flow[BLOCKS] = jnp.zeros((FEATURES, ENTRIES), BF16)
    for owner in range(N_LON):
        pair = blocks_of(outflow_owner, owner)
        for slot in range(CAP):
            index = pair[slot]
            filled = index < BLOCKS
            index = jnp.minimum(index, BLOCKS - 1)
            nodes = outflow_node[pl.ds(index, 1), :].astype(F32)
            pack_out[owner, pl.ds(slot, 1), :] = jnp.where(filled, nodes, -1.0)
            pack_out[owner, pl.ds(2 + slot, 1), :] = outflow_cell[pl.ds(index, 1), :].astype(F32)
            pack_out[owner, pl.ds(4 + slot, 1), :] = outflow_weight[pl.ds(index, 1), :]
        pack_out[owner, pl.ds(6, 2), :] = jnp.zeros((2, ENTRIES), F32)

    for m in range(MEMBERS):
        loads[f"fields{m}"].wait()
        for j in range(ROWS):
            state_a[j, m * CHANNELS : (m + 1) * CHANNELS, :] = tile[
                m, pl.ds(j, CHANNELS, stride=ROWS), :
            ]
    pl.semaphore_wait(barrier, N_LON + 1)

    east, north, mix = wind_east[...], wind_north[...], diffusion[...]
    c_west = jnp.maximum(east, 0.0) + mix
    c_east = mix - jnp.minimum(east, 0.0)
    c_south = jnp.maximum(north, 0.0) + mix
    c_north = mix - jnp.minimum(north, 0.0)
    c_middle = 1.0 - jnp.abs(east) - jnp.abs(north) - 4.0 * mix

    lane = lanes((GROUP, COLS))

    def send_edges(state, step, m):
        rows = slice(m * CHANNELS, (m + 1) * CHANNELS)
        lat_out[step, m, 0] = state[0, rows].astype(BF16)
        lat_out[step, m, 1] = state[ROWS - 1, rows].astype(BF16)

        def collect(g, carry):
            at = pl.ds(pl.multiple_of(m * CHANNELS + g * GROUP, GROUP), GROUP)
            for j in range(ROWS):
                moved = pltpu.roll(state[j, at, :], 16 * g + 2 * j + 1, 1)
                carry = jnp.where(lane // 2 == 8 * g + j, moved, carry)
            return carry

        edge = lax.fori_loop(0, GROUPS, collect, jnp.zeros((GROUP, COLS), F32))
        lon_out[step, m] = edge.astype(BF16)
        return [
            copy(lon_out.at[step, m], lon_in.at[step, m, 1], sides[2]),
            copy(lon_out.at[step, m], lon_in.at[step, m, 0], sides[3]),
            copy(lat_out.at[step, m, 0], lat_in.at[step, m, 1], sides[0]),
            copy(lat_out.at[step, m, 1], lat_in.at[step, m, 0], sides[1]),
        ]

    def advance(state, result, step, m, last):
        from_west = pltpu.roll(lon_in[step, m, 0].astype(F32), 1, 1)
        from_east = pltpu.roll(lon_in[step, m, 1].astype(F32), COLS - 1, 1)
        joined = jnp.where(lane % 2 == 0, from_east, from_west)

        def group(g, carry):
            inner = pl.ds(pl.multiple_of(g * GROUP, GROUP), GROUP)
            at = pl.ds(pl.multiple_of(m * CHANNELS + g * GROUP, GROUP), GROUP)
            low = jnp.where(lat == 0, state[0, at, :], lat_in[step, m, 0, inner, :].astype(F32))
            high = jnp.where(
                lat == N_LAT - 1,
                state[ROWS - 1, at, :],
                lat_in[step, m, 1, inner, :].astype(F32),
            )
            for j in range(ROWS):
                center = state[j, at, :]
                s = low if j == 0 else state[j - 1, at, :]
                n = high if j == ROWS - 1 else state[j + 1, at, :]
                ends = pltpu.roll(joined, 2 * COLS - (16 * g + 2 * j + 1), 1)
                w = jnp.where(lane == 0, ends, pltpu.roll(center, 1, 1))
                e = jnp.where(lane == COLS - 1, ends, pltpu.roll(center, COLS - 1, 1))
                row = slice(j, j + 1)
                value = center * c_middle[row] + w * c_west[row] + e * c_east[row]
                value = value + s * c_south[row] + n * c_north[row]
                result[j, at, :] = value
                if last:
                    grid_bf[at, j * COLS : (j + 1) * COLS] = value.astype(BF16)
            return carry

        lax.fori_loop(0, GROUPS, group, 0)

    def arrive(copies):
        for c in copies:
            c.wait_recv()

    first = [send_edges(state_a, 0, m) for m in range(MEMBERS)]
    wanted = [
        copy(want_out, want_in.at[1], sides[0]),
        copy(want_out, want_in.at[0], sides[1]),
        copy(want_out, want_in.at[3], sides[2]),
        copy(want_out, want_in.at[2], sides[3]),
    ]
    packs = []
    for offset in range(1, N_LON):
        other = (lon + offset) % N_LON
        packs.append(copy(pack_out.at[other], pack_in.at[offset], {"lon": other}))
    pack_in[0] = pack_out[lon]

    def cell_table(k, carry):
        for half in range(2):
            cells = inflow_cell[pl.ds(2 * k + half, 1), :]
            for j in range(ROWS):
                cell_hot[k, j * COLS : (j + 1) * COLS, half * 128 : (half + 1) * 128] = hot(
                    sublanes((COLS, ENTRIES)) + j * COLS == cells
                )
        return carry

    lax.fori_loop(0, BLOCKS // 2, cell_table, 0)
    def edge_table(k, carry):
        at = pl.ds(pl.multiple_of(k * 128, 128), 128)
        senders, receivers = edge_sender[0, :, at], edge_receiver[0, :, at]
        from_column, to_column = column(senders), column(receivers)
        for part_of in range(2):
            spot = lanes((128, 128)) + part_of * 128
            columns = slice(part_of * 128, part_of * 128 + 128)
            edge_hot[at, columns] = hot(from_column == spot)
            edge_hot[at, 256 + part_of * 128 : 384 + part_of * 128] = hot(to_column == spot)
            edge_hot[at, 512 + part_of * 128 : 640 + part_of * 128] = hot(
                from_column == spot + NODES
            )
            collect_hot[columns, at] = hot(sublanes((128, 128)) + part_of * 128 == receivers)
        return carry

    lax.fori_loop(0, EDGES // 128, edge_table, 0)
    second = []
    for m in range(MEMBERS):
        arrive(first[m])
        advance(state_a, state_b, 0, m, False)
        second.append(send_edges(state_b, 1, m))

    def node_table(r, carry):
        node_hot[r] = hot(sublanes((NODES, ENTRIES)) == inflow_node[pl.ds(r, 1), :])
        return carry

    lax.fori_loop(0, BLOCKS, node_table, 0)
    node_hot[BLOCKS] = jnp.zeros((NODES, ENTRIES), BF16)

    def gather(k, carry):
        picked = mm(grid_bf[...], cell_hot[k])
        for half in range(2):
            weights = inflow_weight[pl.ds(2 * k + half, 1), :]
            flow[2 * k + half] = (
                picked[:, half * ENTRIES : (half + 1) * ENTRIES] * weights
            ).astype(BF16)
        return carry

    known = set()

    def share(m, dz, other, rows):
        spot = 2 * (dz % N_Z) + (1 if other else 0)
        if spot not in known:
            known.add(spot)
            owner = 2 * ((z + dz + N_Z) % N_Z) + (1 - y if other else y)
            one, two = in_source[owner * CAP], in_source[owner * CAP + 1]
            values = jnp.concatenate([flow[one], flow[two]], axis=1)
            places = jnp.concatenate([node_hot[one], node_hot[two]], axis=1)
            shares[spot] = nt_dot(values, places)
        return shares[spot, m * CHANNELS + rows.start : m * CHANNELS + rows.stop]

    order = (4, -3, 3, -2, 2, -1, 1, 0)
    hops = ((4, 3), (3, 4), (4, 3))
    lower, upper = slice(0, HALF), slice(HALF, CHANNELS)
    widths = (HALF, HALF, CHANNELS - HALF)

    def reduce_scatter(m):
        y_copies, chains = {}, {}

        def send_y(k):
            rs_y_out[m, k] = share(m, order[k], True, upper).astype(BF16)
            y_copies[k] = copy(rs_y_out.at[m, k], rs_y_in.at[m, k], partner)

        def part(stream, dz):
            if stream < 2:
                return share(m, dz, stream == 0, lower)
            k = order.index(dz)
            y_copies[k].wait_recv()
            return share(m, dz, False, upper) + rs_y_in[m, k].astype(F32)

        def step_z(stream, s):
            for way in range(2):
                length = hops[stream][way]
                if s >= length:
                    continue
                dz = (length - s) * (1 if way == 0 else -1)
                value = part(stream, dz)
                if s:
                    chains[stream, way, s - 1].wait_recv()
                    value = value + rs_in[m, stream, way, s - 1, : widths[stream]].astype(F32)
                width = widths[stream]
                rs_out[m, stream, way, s, :width] = value.astype(BF16)
                chains[stream, way, s] = copy(
                    rs_out.at[m, stream, way, s, pl.ds(0, width)],
                    rs_in.at[m, stream, way, s, pl.ds(0, width)],
                    above if way == 0 else below,
                )

        def end_z(stream):
            value = part(stream, 0)
            for way in range(2):
                last = hops[stream][way] - 1
                chains[stream, way, last].wait_recv()
                value = value + rs_in[m, stream, way, last, : widths[stream]].astype(F32)
            return value

        def begin():
            send_y(0)
            send_y(1)
            step_z(0, 0)
            step_z(1, 0)

        def rest_y():
            for k in range(2, 8):
                send_y(k)

        last_y = []

        def end_first():
            rs_last_out[m] = end_z(0).astype(BF16)
            last_y.append(copy(rs_last_out.at[m], rs_last_in.at[m], partner))

        def end_others():
            node_input[m, lower] = end_z(1)
            node_input[m, upper] = end_z(2)

        def end():
            arrive(last_y)
            node_input[m, lower] += rs_last_in[m].astype(F32)

        return begin, rest_y, step_z, end_first, end_others, end

    def run(work, count=1):
        for _ in range(count):
            next(work, None)

    def finish(work):
        for _ in work:
            pass

    def network(m):
        turned = jnp.transpose(
            jnp.concatenate([node_input[m], jnp.zeros((64, NODES), F32)], axis=0)
        )[:, :CHANNELS].astype(BF16)
        hidden[m] = silu(mm(turned, encoder[...]))
        yield
        for layer in range(LAYERS):
            normed = normalize(hidden[m])
            source_target[m, :NODES] = mm(normed, sender_w[layer]).astype(BF16)
            travelling = []
            for q in (2, 3, 0, 1):
                halo_out[m, layer, q] = mm(want_hot[q], source_target[m, :NODES]).astype(BF16)
                travelling.append(
                    copy(
                        halo_out.at[m, layer, q],
                        halo.at[m, layer, pl.ds((q ^ 1) * HCAP, HCAP)],
                        sides[q],
                    )
                )
            yield
            source_target[m, NODES:] = mm(normed, receiver_w[layer]).astype(BF16)
            for k in range(3):
                at = slice(k * 512, (k + 1) * 512)
                summed[m, at] = mm(edge_hot[at, : 2 * NODES], source_target[m])
                yield
            arrive(travelling)
            for k in range(3):
                at = slice(k * 512, (k + 1) * 512)
                value = summed[m, at] + mm(edge_hot[at, 2 * NODES :], halo[m, layer])
                message[m, at] = silu(value).astype(BF16)
                yield
            collected = mm(collect_hot[...], message[m]).astype(BF16)
            hidden[m] += mm(collected, update_w[layer])
            yield
        both[m, 0, 0] = nt_dot(decoder[...], normalize(hidden[m])).astype(BF16)

    lengths = ((3, 4), (4, 3), (4, 3))
    low_half, high_half = pl.ds(0, HALF), pl.ds(HALF, CHANNELS - HALF)

    def slot_of(way, s):
        return s if way == 0 else (N_Z - s) % N_Z

    def gather_all(m):
        moves, y_moves = {}, {}

        def view(stream, slot):
            return both.at[m, stream % 2, slot, high_half if stream == 2 else low_half]

        def pass_y(slot):
            y_moves[slot] = copy(
                both.at[m, 0, slot, high_half], both.at[m, 1, slot, high_half], partner
            )

        def forward(stream, s):
            for way in range(2):
                if s and s <= lengths[stream][way]:
                    moves[stream, way, s - 1].wait_recv()
                    if stream == 2:
                        pass_y(slot_of(way, s))
                if s < lengths[stream][way]:
                    moves[stream, way, s] = copy(
                        view(stream, slot_of(way, s)),
                        view(stream, slot_of(way, s + 1)),
                        above if way == 0 else below,
                    )

        def add(side, slots):
            total = None
            for slot in slots:
                if side:
                    y_moves[slot].wait_recv()
                    k = (2 * slot + 2 * y + N_LON - 1) % N_LON
                else:
                    k = 2 * slot
                term = mm(both[m, side, slot], spread[k])
                total = term if total is None else total + term
            adjust[m] += total

        across = []

        def begin():
            across.append(copy(view(0, 0), view(1, 0), partner))
            forward(2, 0)
            forward(0, 0)
            pass_y(0)

        def begin_other():
            arrive(across)
            forward(1, 0)

        def end():
            for j in range(ROWS):
                tile[m, pl.ds(j, CHANNELS, stride=ROWS), :] = adjust[
                    m, :, j * COLS : (j + 1) * COLS
                ]
            done = pltpu.make_async_copy(tile.at[m], out_hbm.at[m], load_sem.at[7 + m])
            done.start()
            results.append(done)

        return begin, begin_other, forward, add, end

    results = []

    def wanted_table():
        arrive(wanted)
        for q in range(4):
            rows = column(want_in[q, (q ^ 1) : (q ^ 1) + 1, :])[:HCAP]
            for part_of in range(2):
                want_hot[q, :, part_of * 128 : part_of * 128 + 128] = hot(
                    rows == lanes((HCAP, 128)) + part_of * 128
                )
        for m in range(MEMBERS):
            for layer in range(LAYERS):
                halo[m, layer, 4 * HCAP :] = jnp.zeros((NODES - 4 * HCAP, HID), BF16)

    def spread_table(k, carry):
        rows = pack_in[k]
        spot = sublanes((NODES, ENTRIES)).astype(F32)
        weights, places = [], []
        for slot in range(CAP):
            weights.append(
                jnp.where(spot == rows[slot : slot + 1], rows[4 + slot : 5 + slot], 0.0).astype(BF16)
            )
        weighted = jnp.concatenate(weights, axis=1)
        for j in range(4):
            places = [
                hot(spot + j * NODES == rows[2 + slot : 3 + slot]) for slot in range(CAP)
            ]
            spread[k, :, j * NODES : (j + 1) * NODES] = nt_dot(
                weighted, jnp.concatenate(places, axis=1)
            ).astype(BF16)
        return carry

    arrive(packs)
    wanted_table()
    lax.fori_loop(0, 4, spread_table, 0)
    for m in range(MEMBERS):
        arrive(second[m])
        advance(state_b, state_a, 1, m, True)
    lax.fori_loop(0, BLOCKS // 2, gather, 0)
    sums = [reduce_scatter(m) for m in range(MEMBERS)]
    begin0, rest0, step0, first0, others0, end0 = sums[0]
    begin1, rest1, step1, first1, others1, end1 = sums[1]
    begin0()
    begin1()
    rest0()
    lax.fori_loop(4, 8, spread_table, 0)
    step0(2, 0)
    rest1()
    step0(0, 1)
    step0(1, 1)
    step1(0, 1)
    step1(1, 1)
    step1(2, 0)
    lax.fori_loop(8, 12, spread_table, 0)
    step0(2, 1)
    step0(0, 2)
    step0(1, 2)
    step1(0, 2)
    step1(1, 2)
    lax.fori_loop(12, 16, spread_table, 0)
    step0(2, 2)
    step0(0, 3)
    step0(1, 3)
    step1(2, 1)
    step1(0, 3)
    step1(1, 3)
    for name in ("encoder", "sender", "receiver", "update", "decoder"):
        loads[name].wait()
    step0(2, 3)
    first0()
    step1(2, 2)
    first1()
    others0()
    end0()
    nets = [network(m) for m in range(MEMBERS)]
    net0, net1 = nets
    start_a, other_a, pass_a, add_a, end_a = gather_all(0)
    start_b, other_b, pass_b, add_b, end_b = gather_all(1)
    run(net0, 2)
    step1(2, 3)
    run(net0, 3)
    others1()
    end1()
    run(net1, 2)
    run(net1, 3)
    run(net0)
    run(net0, 4)
    run(net1)
    run(net1, 4)
    run(net0, 3)
    run(net0)
    finish(net0)
    start_a()
    for m in range(MEMBERS):
        for j in range(ROWS):
            adjust[m, :, j * COLS : (j + 1) * COLS] = state_a[
                j, m * CHANNELS : (m + 1) * CHANNELS, :
            ]
    run(net1, 3)
    run(net1)
    finish(net1)
    start_b()
    other_a()
    pass_a(2, 1)
    pass_a(0, 1)
    add_a(0, [0])
    add_b(0, [0])
    other_b()
    pass_b(2, 1)
    pass_b(0, 1)
    pass_a(2, 2)
    pass_a(1, 1)
    pass_a(0, 2)
    add_a(1, [0])
    pass_b(2, 2)
    pass_b(1, 1)
    pass_b(0, 2)
    add_a(0, [1, 7])
    add_b(1, [0])
    pass_a(2, 3)
    pass_a(1, 2)
    pass_a(0, 3)
    add_a(1, [1, 7])
    add_b(0, [1, 7])
    pass_b(2, 3)
    pass_b(1, 2)
    pass_b(0, 3)
    add_b(1, [1, 7])
    add_a(0, [2, 6])
    pass_a(2, 4)
    pass_a(1, 3)
    pass_a(0, 4)
    add_a(1, [2, 6])
    add_a(0, [3, 5])
    add_a(0, [4])
    add_b(0, [2, 6])
    pass_b(2, 4)
    pass_b(1, 3)
    pass_b(0, 4)
    add_b(1, [2, 6])
    add_b(0, [3, 5])
    add_b(0, [4])
    pass_a(1, 4)
    add_a(1, [3, 5])
    add_a(1, [4])
    end_a()
    pass_b(1, 4)
    add_b(1, [3, 5])
    add_b(1, [4])
    end_b()
    for c in started:
        c.wait_send()
    for c in results:
        c.wait()


def body(
    fields,
    wind_east,
    wind_north,
    diffusion,
    inflow_owner,
    inflow_cell,
    inflow_node,
    inflow_weight,
    encoder,
    sender_weight,
    receiver_weight,
    update_weight,
    decoder,
    edge_sender,
    edge_receiver,
    halo_rows,
    outflow_owner,
    outflow_node,
    outflow_cell,
    outflow_weight,
):
    vmem = pl.BlockSpec(memory_space=pltpu.VMEM)
    smem = pl.BlockSpec(memory_space=pltpu.SMEM)
    anywhere = pl.BlockSpec(memory_space=pl.ANY)
    half = (CHANNELS - HALF, NODES)
    scratch = [
        pltpu.VMEM((MEMBERS, CHANNELS * ROWS, COLS), F32),
        pltpu.VMEM((ROWS, FEATURES, COLS), F32),
        pltpu.VMEM((ROWS, FEATURES, COLS), F32),
        pltpu.VMEM((DSTEPS, MEMBERS, 2, CHANNELS, COLS), BF16),
        pltpu.VMEM((DSTEPS, MEMBERS, 2, CHANNELS, COLS), BF16),
        pltpu.VMEM((DSTEPS, MEMBERS, GROUP, COLS), BF16),
        pltpu.VMEM((DSTEPS, MEMBERS, 2, GROUP, COLS), BF16),
        pltpu.VMEM((FEATURES, CELLS), BF16),
        pltpu.VMEM((BLOCKS // 2, CELLS, 2 * ENTRIES), BF16),
        pltpu.VMEM((BLOCKS + 1, FEATURES, ENTRIES), BF16),
        pltpu.VMEM((BLOCKS + 1, NODES, ENTRIES), BF16),
        pltpu.VMEM((N_LON, 8, ENTRIES), F32),
        pltpu.VMEM((N_LON, 8, ENTRIES), F32),
        pltpu.VMEM((4, 8, 128), jnp.int32),
        pltpu.VMEM((N_LON, FEATURES, NODES), F32),
        pltpu.VMEM((MEMBERS, 3, 2, 4) + half, BF16),
        pltpu.VMEM((MEMBERS, 3, 2, 4) + half, BF16),
        pltpu.VMEM((MEMBERS, N_Z) + half, BF16),
        pltpu.VMEM((MEMBERS, N_Z) + half, BF16),
        pltpu.VMEM((MEMBERS, HALF, NODES), BF16),
        pltpu.VMEM((MEMBERS, HALF, NODES), BF16),
        pltpu.VMEM((MEMBERS, CHANNELS, NODES), F32),
        pltpu.VMEM((EDGES, 3 * NODES), BF16),
        pltpu.VMEM((NODES, EDGES), BF16),
        pltpu.VMEM((4, HCAP, NODES), BF16),
        pltpu.VMEM((CHANNELS, HID), BF16),
        pltpu.VMEM((LAYERS, HID, HID), BF16),
        pltpu.VMEM((LAYERS, HID, HID), BF16),
        pltpu.VMEM((LAYERS, HID, HID), BF16),
        pltpu.VMEM((CHANNELS, HID), BF16),
        pltpu.VMEM((MEMBERS, NODES, HID), F32),
        pltpu.VMEM((MEMBERS, 2 * NODES, HID), BF16),
        pltpu.VMEM((MEMBERS, LAYERS, 4, HCAP, HID), BF16),
        pltpu.VMEM((MEMBERS, LAYERS, NODES, HID), BF16),
        pltpu.VMEM((MEMBERS, EDGES, HID), F32),
        pltpu.VMEM((MEMBERS, EDGES, HID), BF16),
        pltpu.VMEM((N_LON, NODES, CELLS), BF16),
        pltpu.VMEM((MEMBERS, 2, N_Z, CHANNELS, NODES), BF16),
        pltpu.VMEM((MEMBERS, CHANNELS, CELLS), F32),
        pltpu.SMEM((N_LON * CAP,), jnp.int32),
        pltpu.VMEM((8, 128), jnp.int32),
        pltpu.SemaphoreType.DMA((9,)),
        pltpu.SemaphoreType.DMA((COPIES,)),
        pltpu.SemaphoreType.DMA((COPIES,)),
    ]
    result = pl.pallas_call(
        kernel,
        out_shape=jax.ShapeDtypeStruct((MEMBERS, CHANNELS * ROWS, COLS), F32),
        in_specs=[smem, smem, anywhere]
        + [vmem] * 6
        + [anywhere] * 5
        + [vmem] * 6,
        out_specs=anywhere,
        scratch_shapes=scratch,
        compiler_params=pltpu.CompilerParams(
            collective_id=0, has_side_effects=True, vmem_limit_bytes=VMEM_LIMIT
        ),
    )(
        inflow_owner.reshape(1, BLOCKS),
        outflow_owner.reshape(1, BLOCKS),
        fields.reshape(MEMBERS, CHANNELS * ROWS, COLS),
        wind_east,
        wind_north,
        diffusion,
        inflow_cell,
        inflow_node,
        inflow_weight,
        encoder,
        sender_weight,
        receiver_weight,
        update_weight,
        decoder.T,
        edge_sender,
        edge_receiver,
        halo_rows,
        outflow_node,
        outflow_cell,
        outflow_weight,
    )
    return result.reshape(MEMBERS, CHANNELS, ROWS, COLS)


def solution(mesh):
    placed = (
        P("member", None, "lat", "lon"),
        P("lat", "lon"),
        P("lat", "lon"),
        P("lat", "lon"),
        P(("lat", "lon"), None),
        P(("lat", "lon"), None),
        P(("lat", "lon"), None),
        P(("lat", "lon"), None),
        P(),
        P(),
        P(),
        P(),
        P(),
        P("lat", "lon", None),
        P("lat", "lon", None),
        P("lat", "lon", None, None),
        P(("lat", "lon"), None),
        P(("lat", "lon"), None),
        P(("lat", "lon"), None),
        P(("lat", "lon"), None),
    )
    return jax.shard_map(
        body, mesh=mesh, in_specs=placed, out_specs=P("member", None, "lat", "lon"), check_vma=False
    )
```

```python
import jax
import jax.numpy as jnp
from jax import lax
from jax.experimental import pallas as pl
from jax.experimental.pallas import tpu as pltpu
from jax.sharding import PartitionSpec as P

F32, BF16 = jnp.float32, jnp.bfloat16
MESH = pl.DeviceIdType.MESH
MEMBERS = 2
CHANNELS = 192
FEATURES = MEMBERS * CHANNELS
ROWS, COLS = 8, 128
CELLS = ROWS * COLS
BLOCKS, ENTRIES, CAP = 16, 128, 2
NODES = 256
HCAP = 48
EDGES = 1536
HID = 512
LAYERS = 2
DSTEPS = 2
N_LAT, N_LON = 8, 16
N_Z = N_LON // 2
GROUP = 48
GROUPS = CHANNELS // GROUP
HALF = 80
COPIES = 192
VMEM_LIMIT = 63 * 1024 * 1024


def nt_dot(a, b):
    return lax.dot_general(a, b, (((1,), (1,)), ((), ())), preferred_element_type=F32)


def mm(a, b):
    return jnp.dot(a, b, preferred_element_type=F32)


def hot(mask):
    return jnp.where(mask, 1.0, 0.0).astype(BF16)


def silu(v):
    half = 0.5 * v
    return half + half * jnp.tanh(half)


def normalize(values):
    scale = lax.rsqrt(jnp.mean(values * values, axis=-1, keepdims=True) + 1e-06)
    return (values * scale).astype(BF16)


def lanes(shape):
    return lax.broadcasted_iota(jnp.int32, shape, 1)


def sublanes(shape):
    return lax.broadcasted_iota(jnp.int32, shape, 0)


def column(row):
    return jnp.transpose(jnp.broadcast_to(row.astype(F32), (128, 128))).astype(jnp.int32)


def kernel(
    inflow_owner,
    outflow_owner,
    fields_hbm,
    wind_east,
    wind_north,
    diffusion,
    inflow_cell,
    inflow_node,
    inflow_weight,
    encoder_hbm,
    sender_hbm,
    receiver_hbm,
    update_hbm,
    decoder_hbm,
    edge_sender,
    edge_receiver,
    halo_rows,
    outflow_node,
    outflow_cell,
    outflow_weight,
    out_hbm,
    tile,
    state_a,
    state_b,
    lat_out,
    lat_in,
    lon_out,
    lon_in,
    grid_bf,
    cell_hot,
    flow,
    node_hot,
    pack_out,
    pack_in,
    want_in,
    shares,
    rs_out,
    rs_in,
    rs_y_out,
    rs_y_in,
    rs_last_out,
    rs_last_in,
    node_input,
    edge_hot,
    collect_hot,
    want_hot,
    encoder,
    sender_w,
    receiver_w,
    update_w,
    decoder,
    hidden,
    source_target,
    halo_out,
    halo,
    summed,
    message,
    spread,
    both,
    adjust,
    in_source,
    want_out,
    load_sem,
    send_sem,
    recv_sem,
):
    lat = lax.axis_index("lat")
    lon = lax.axis_index("lon")
    z, y = lon // 2, lon % 2
    sides = (
        {"lat": (lat + N_LAT - 1) % N_LAT},
        {"lat": (lat + 1) % N_LAT},
        {"lon": (lon + N_LON - 1) % N_LON},
        {"lon": (lon + 1) % N_LON},
    )
    above = {"lon": (lon + 2) % N_LON}
    below = {"lon": (lon + N_LON - 2) % N_LON}
    partner = {"lon": 2 * z + (1 - y)}
    used = [0]
    started = []

    def copy(src, dst, device):
        index = used[0]
        used[0] += 1
        made = pltpu.make_async_remote_copy(
            src_ref=src,
            dst_ref=dst,
            send_sem=send_sem.at[index],
            recv_sem=recv_sem.at[index],
            device_id=device,
            device_id_type=MESH,
        )
        made.start()
        started.append(made)
        return made

    loads = {}
    for index, (name, src, dst) in enumerate(
        (
            ("fields0", fields_hbm.at[0], tile.at[0]),
            ("fields1", fields_hbm.at[1], tile.at[1]),
            ("encoder", encoder_hbm, encoder),
            ("sender", sender_hbm, sender_w),
            ("receiver", receiver_hbm, receiver_w),
            ("update", update_hbm, update_w),
            ("decoder", decoder_hbm, decoder),
        )
    ):
        loads[name] = pltpu.make_async_copy(src, dst, load_sem.at[index])
        loads[name].start()

    barrier = pltpu.get_barrier_semaphore()
    for side in sides[:2]:
        pl.semaphore_signal(barrier, inc=1, device_id=side, device_id_type=MESH)
    for offset in range(1, N_LON):
        pl.semaphore_signal(
            barrier, inc=1, device_id={"lon": (lon + offset) % N_LON}, device_id_type=MESH
        )

    def blocks_of(owners, owner):
        first, second = jnp.int32(BLOCKS), jnp.int32(BLOCKS)
        for r in reversed(range(BLOCKS)):
            same = owners[0, r] == owner
            second = jnp.where(same, first, second)
            first = jnp.where(same, r, first)
        return first, second

    for owner in range(N_LON):
        pair = blocks_of(inflow_owner, owner)
        for slot in range(CAP):
            in_source[owner * CAP + slot] = pair[slot]
    want_out[...] = jnp.zeros((8, 128), jnp.int32)
    want_out[:4, :HCAP] = halo_rows[0, 0]

    flow[BLOCKS] = jnp.zeros((FEATURES, ENTRIES), BF16)
    for owner in range(N_LON):
        pair = blocks_of(outflow_owner, owner)
        for slot in range(CAP):
            index = pair[slot]
            filled = index < BLOCKS
            index = jnp.minimum(index, BLOCKS - 1)
            nodes = outflow_node[pl.ds(index, 1), :].astype(F32)
            pack_out[owner, pl.ds(slot, 1), :] = jnp.where(filled, nodes, -1.0)
            pack_out[owner, pl.ds(2 + slot, 1), :] = outflow_cell[pl.ds(index, 1), :].astype(F32)
            pack_out[owner, pl.ds(4 + slot, 1), :] = outflow_weight[pl.ds(index, 1), :]
        pack_out[owner, pl.ds(6, 2), :] = jnp.zeros((2, ENTRIES), F32)

    for m in range(MEMBERS):
        loads[f"fields{m}"].wait()
        for j in range(ROWS):
            state_a[j, m * CHANNELS : (m + 1) * CHANNELS, :] = tile[
                m, pl.ds(j, CHANNELS, stride=ROWS), :
            ]
    pl.semaphore_wait(barrier, N_LON + 1)

    east, north, mix = wind_east[...], wind_north[...], diffusion[...]
    c_west = jnp.maximum(east, 0.0) + mix
    c_east = mix - jnp.minimum(east, 0.0)
    c_south = jnp.maximum(north, 0.0) + mix
    c_north = mix - jnp.minimum(north, 0.0)
    c_middle = 1.0 - jnp.abs(east) - jnp.abs(north) - 4.0 * mix

    lane = lanes((GROUP, COLS))

    def send_edges(state, step, m):
        rows = slice(m * CHANNELS, (m + 1) * CHANNELS)
        lat_out[step, m, 0] = state[0, rows].astype(BF16)
        lat_out[step, m, 1] = state[ROWS - 1, rows].astype(BF16)

        def collect(g, carry):
            at = pl.ds(pl.multiple_of(m * CHANNELS + g * GROUP, GROUP), GROUP)
            for j in range(ROWS):
                moved = pltpu.roll(state[j, at, :], 16 * g + 2 * j + 1, 1)
                carry = jnp.where(lane // 2 == 8 * g + j, moved, carry)
            return carry

        edge = lax.fori_loop(0, GROUPS, collect, jnp.zeros((GROUP, COLS), F32), unroll=2)
        lon_out[step, m] = edge.astype(BF16)
        return [
            copy(lon_out.at[step, m], lon_in.at[step, m, 1], sides[2]),
            copy(lon_out.at[step, m], lon_in.at[step, m, 0], sides[3]),
            copy(lat_out.at[step, m, 0], lat_in.at[step, m, 1], sides[0]),
            copy(lat_out.at[step, m, 1], lat_in.at[step, m, 0], sides[1]),
        ]

    def advance(state, result, step, m, last):
        from_west = pltpu.roll(lon_in[step, m, 0].astype(F32), 1, 1)
        from_east = pltpu.roll(lon_in[step, m, 1].astype(F32), COLS - 1, 1)
        joined = jnp.where(lane % 2 == 0, from_east, from_west)

        def group(g, carry):
            inner = pl.ds(pl.multiple_of(g * GROUP, GROUP), GROUP)
            at = pl.ds(pl.multiple_of(m * CHANNELS + g * GROUP, GROUP), GROUP)
            low = jnp.where(lat == 0, state[0, at, :], lat_in[step, m, 0, inner, :].astype(F32))
            high = jnp.where(
                lat == N_LAT - 1,
                state[ROWS - 1, at, :],
                lat_in[step, m, 1, inner, :].astype(F32),
            )
            for j in range(ROWS):
                center = state[j, at, :]
                s = low if j == 0 else state[j - 1, at, :]
                n = high if j == ROWS - 1 else state[j + 1, at, :]
                ends = pltpu.roll(joined, 2 * COLS - (16 * g + 2 * j + 1), 1)
                w = jnp.where(lane == 0, ends, pltpu.roll(center, 1, 1))
                e = jnp.where(lane == COLS - 1, ends, pltpu.roll(center, COLS - 1, 1))
                row = slice(j, j + 1)
                value = center * c_middle[row] + w * c_west[row] + e * c_east[row]
                value = value + s * c_south[row] + n * c_north[row]
                result[j, at, :] = value
                if last:
                    grid_bf[at, j * COLS : (j + 1) * COLS] = value.astype(BF16)
            return carry

        lax.fori_loop(0, GROUPS, group, 0, unroll=2)

    def arrive(copies):
        for c in copies:
            c.wait_recv()

    first = [send_edges(state_a, 0, m) for m in range(MEMBERS)]
    wanted = [
        copy(want_out, want_in.at[1], sides[0]),
        copy(want_out, want_in.at[0], sides[1]),
        copy(want_out, want_in.at[3], sides[2]),
        copy(want_out, want_in.at[2], sides[3]),
    ]
    packs = []
    for offset in range(1, N_LON):
        other = (lon + offset) % N_LON
        packs.append(copy(pack_out.at[other], pack_in.at[offset], {"lon": other}))
    pack_in[0] = pack_out[lon]

    def cell_table(k, carry):
        for half in range(2):
            cells = inflow_cell[pl.ds(2 * k + half, 1), :]
            for j in range(ROWS):
                cell_hot[k, j * COLS : (j + 1) * COLS, half * 128 : (half + 1) * 128] = hot(
                    sublanes((COLS, ENTRIES)) + j * COLS == cells
                )
        return carry

    lax.fori_loop(0, BLOCKS // 2, cell_table, 0)
    def edge_table(k, carry):
        at = pl.ds(pl.multiple_of(k * 128, 128), 128)
        senders, receivers = edge_sender[0, :, at], edge_receiver[0, :, at]
        from_column, to_column = column(senders), column(receivers)
        for part_of in range(2):
            spot = lanes((128, 128)) + part_of * 128
            columns = slice(part_of * 128, part_of * 128 + 128)
            edge_hot[at, columns] = hot(from_column == spot)
            edge_hot[at, 256 + part_of * 128 : 384 + part_of * 128] = hot(to_column == spot)
            edge_hot[at, 512 + part_of * 128 : 640 + part_of * 128] = hot(
                from_column == spot + NODES
            )
            collect_hot[columns, at] = hot(sublanes((128, 128)) + part_of * 128 == receivers)
        return carry

    lax.fori_loop(0, EDGES // 128, edge_table, 0)
    second = []
    for m in range(MEMBERS):
        arrive(first[m])
        advance(state_a, state_b, 0, m, False)
        second.append(send_edges(state_b, 1, m))

    def node_table(r, carry):
        node_hot[r] = hot(sublanes((NODES, ENTRIES)) == inflow_node[pl.ds(r, 1), :])
        return carry

    lax.fori_loop(0, BLOCKS, node_table, 0)
    node_hot[BLOCKS] = jnp.zeros((NODES, ENTRIES), BF16)

    def gather(k, carry):
        picked = mm(grid_bf[...], cell_hot[k])
        for half in range(2):
            weights = inflow_weight[pl.ds(2 * k + half, 1), :]
            flow[2 * k + half] = (
                picked[:, half * ENTRIES : (half + 1) * ENTRIES] * weights
            ).astype(BF16)
        return carry

    known = set()

    def share(m, dz, other, rows):
        spot = 2 * (dz % N_Z) + (1 if other else 0)
        if spot not in known:
            known.add(spot)
            owner = 2 * ((z + dz + N_Z) % N_Z) + (1 - y if other else y)
            one, two = in_source[owner * CAP], in_source[owner * CAP + 1]
            values = jnp.concatenate([flow[one], flow[two]], axis=1)
            places = jnp.concatenate([node_hot[one], node_hot[two]], axis=1)
            shares[spot] = nt_dot(values, places)
        return shares[spot, m * CHANNELS + rows.start : m * CHANNELS + rows.stop]

    order = (4, -3, 3, -2, 2, -1, 1, 0)
    hops = ((4, 3), (3, 4), (4, 3))
    lower, upper = slice(0, HALF), slice(HALF, CHANNELS)
    widths = (HALF, HALF, CHANNELS - HALF)

    def reduce_scatter(m):
        y_copies, chains = {}, {}

        def send_y(k):
            rs_y_out[m, k] = share(m, order[k], True, upper).astype(BF16)
            y_copies[k] = copy(rs_y_out.at[m, k], rs_y_in.at[m, k], partner)

        def part(stream, dz):
            if stream < 2:
                return share(m, dz, stream == 0, lower)
            k = order.index(dz)
            y_copies[k].wait_recv()
            return share(m, dz, False, upper) + rs_y_in[m, k].astype(F32)

        def step_z(stream, s):
            for way in range(2):
                length = hops[stream][way]
                if s >= length:
                    continue
                dz = (length - s) * (1 if way == 0 else -1)
                value = part(stream, dz)
                if s:
                    chains[stream, way, s - 1].wait_recv()
                    value = value + rs_in[m, stream, way, s - 1, : widths[stream]].astype(F32)
                width = widths[stream]
                rs_out[m, stream, way, s, :width] = value.astype(BF16)
                chains[stream, way, s] = copy(
                    rs_out.at[m, stream, way, s, pl.ds(0, width)],
                    rs_in.at[m, stream, way, s, pl.ds(0, width)],
                    above if way == 0 else below,
                )

        def end_z(stream):
            value = part(stream, 0)
            for way in range(2):
                last = hops[stream][way] - 1
                chains[stream, way, last].wait_recv()
                value = value + rs_in[m, stream, way, last, : widths[stream]].astype(F32)
            return value

        def begin():
            send_y(0)
            send_y(1)
            step_z(0, 0)
            step_z(1, 0)

        def rest_y():
            for k in range(2, 8):
                send_y(k)

        last_y = []

        def end_first():
            rs_last_out[m] = end_z(0).astype(BF16)
            last_y.append(copy(rs_last_out.at[m], rs_last_in.at[m], partner))

        def end_others():
            node_input[m, lower] = end_z(1)
            node_input[m, upper] = end_z(2)

        def end():
            arrive(last_y)
            node_input[m, lower] += rs_last_in[m].astype(F32)

        return begin, rest_y, step_z, end_first, end_others, end

    def run(work, count=1):
        for _ in range(count):
            next(work, None)

    def finish(work):
        for _ in work:
            pass

    def network(m):
        turned = jnp.transpose(
            jnp.concatenate([node_input[m], jnp.zeros((64, NODES), F32)], axis=0)
        )[:, :CHANNELS].astype(BF16)
        hidden[m] = silu(mm(turned, encoder[...]))
        yield
        for layer in range(LAYERS):
            normed = normalize(hidden[m])
            source_target[m, :NODES] = mm(normed, sender_w[layer]).astype(BF16)
            travelling = []
            for q in (2, 3, 0, 1):
                halo_out[m, layer, q] = mm(want_hot[q], source_target[m, :NODES]).astype(BF16)
                travelling.append(
                    copy(
                        halo_out.at[m, layer, q],
                        halo.at[m, layer, pl.ds((q ^ 1) * HCAP, HCAP)],
                        sides[q],
                    )
                )
            yield
            source_target[m, NODES:] = mm(normed, receiver_w[layer]).astype(BF16)
            for k in range(3):
                at = slice(k * 512, (k + 1) * 512)
                summed[m, at] = mm(edge_hot[at, : 2 * NODES], source_target[m])
                yield
            arrive(travelling)
            for k in range(3):
                at = slice(k * 512, (k + 1) * 512)
                value = summed[m, at] + mm(edge_hot[at, 2 * NODES :], halo[m, layer])
                message[m, at] = silu(value).astype(BF16)
                yield
            collected = mm(collect_hot[...], message[m]).astype(BF16)
            hidden[m] += mm(collected, update_w[layer])
            yield
        both[m, 0, 0] = nt_dot(decoder[...], normalize(hidden[m])).astype(BF16)

    lengths = ((3, 4), (4, 3), (4, 3))
    low_half, high_half = pl.ds(0, HALF), pl.ds(HALF, CHANNELS - HALF)

    def slot_of(way, s):
        return s if way == 0 else (N_Z - s) % N_Z

    def gather_all(m):
        moves, y_moves = {}, {}

        def view(stream, slot):
            return both.at[m, stream % 2, slot, high_half if stream == 2 else low_half]

        def pass_y(slot):
            y_moves[slot] = copy(
                both.at[m, 0, slot, high_half], both.at[m, 1, slot, high_half], partner
            )

        def forward(stream, s):
            for way in range(2):
                if s and s <= lengths[stream][way]:
                    moves[stream, way, s - 1].wait_recv()
                    if stream == 2:
                        pass_y(slot_of(way, s))
                if s < lengths[stream][way]:
                    moves[stream, way, s] = copy(
                        view(stream, slot_of(way, s)),
                        view(stream, slot_of(way, s + 1)),
                        above if way == 0 else below,
                    )

        def add(side, slots):
            total = None
            for slot in slots:
                if side:
                    y_moves[slot].wait_recv()
                    k = (2 * slot + 2 * y + N_LON - 1) % N_LON
                else:
                    k = 2 * slot
                term = mm(both[m, side, slot], spread[k])
                total = term if total is None else total + term
            adjust[m] += total

        across = []

        def begin():
            across.append(copy(view(0, 0), view(1, 0), partner))
            forward(2, 0)
            forward(0, 0)
            pass_y(0)

        def begin_other():
            arrive(across)
            forward(1, 0)

        def end():
            for j in range(ROWS):
                tile[m, pl.ds(j, CHANNELS, stride=ROWS), :] = adjust[
                    m, :, j * COLS : (j + 1) * COLS
                ]
            done = pltpu.make_async_copy(tile.at[m], out_hbm.at[m], load_sem.at[7 + m])
            done.start()
            results.append(done)

        return begin, begin_other, forward, add, end

    results = []

    def wanted_table():
        arrive(wanted)
        for q in range(4):
            rows = column(want_in[q, (q ^ 1) : (q ^ 1) + 1, :])[:HCAP]
            for part_of in range(2):
                want_hot[q, :, part_of * 128 : part_of * 128 + 128] = hot(
                    rows == lanes((HCAP, 128)) + part_of * 128
                )
        for m in range(MEMBERS):
            for layer in range(LAYERS):
                halo[m, layer, 4 * HCAP :] = jnp.zeros((NODES - 4 * HCAP, HID), BF16)

    def spread_table(k, carry):
        rows = pack_in[k]
        spot = sublanes((NODES, ENTRIES)).astype(F32)
        weights, places = [], []
        for slot in range(CAP):
            weights.append(
                jnp.where(spot == rows[slot : slot + 1], rows[4 + slot : 5 + slot], 0.0).astype(BF16)
            )
        weighted = jnp.concatenate(weights, axis=1)
        for j in range(4):
            places = [
                hot(spot + j * NODES == rows[2 + slot : 3 + slot]) for slot in range(CAP)
            ]
            spread[k, :, j * NODES : (j + 1) * NODES] = nt_dot(
                weighted, jnp.concatenate(places, axis=1)
            ).astype(BF16)
        return carry

    arrive(packs)
    wanted_table()
    lax.fori_loop(0, 4, spread_table, 0)
    for m in range(MEMBERS):
        arrive(second[m])
        advance(state_b, state_a, 1, m, True)
    lax.fori_loop(0, BLOCKS // 2, gather, 0, unroll=4)
    sums = [reduce_scatter(m) for m in range(MEMBERS)]
    begin0, rest0, step0, first0, others0, end0 = sums[0]
    begin1, rest1, step1, first1, others1, end1 = sums[1]
    begin0()
    begin1()
    rest0()
    lax.fori_loop(4, 8, spread_table, 0)
    step0(2, 0)
    rest1()
    step0(0, 1)
    step0(1, 1)
    step1(0, 1)
    step1(1, 1)
    step1(2, 0)
    lax.fori_loop(8, 12, spread_table, 0)
    step0(2, 1)
    step0(0, 2)
    step0(1, 2)
    step1(0, 2)
    step1(1, 2)
    lax.fori_loop(12, 16, spread_table, 0)
    step0(2, 2)
    step0(0, 3)
    step0(1, 3)
    step1(2, 1)
    step1(0, 3)
    step1(1, 3)
    for name in ("encoder", "sender", "receiver", "update", "decoder"):
        loads[name].wait()
    step0(2, 3)
    first0()
    step1(2, 2)
    first1()
    others0()
    end0()
    nets = [network(m) for m in range(MEMBERS)]
    net0, net1 = nets
    start_a, other_a, pass_a, add_a, end_a = gather_all(0)
    start_b, other_b, pass_b, add_b, end_b = gather_all(1)
    run(net0, 2)
    step1(2, 3)
    run(net0, 3)
    others1()
    end1()
    run(net1, 2)
    run(net1, 3)
    run(net0)
    run(net0, 4)
    run(net1)
    run(net1, 4)
    run(net0, 3)
    run(net0)
    finish(net0)
    start_a()
    for m in range(MEMBERS):
        for j in range(ROWS):
            adjust[m, :, j * COLS : (j + 1) * COLS] = state_a[
                j, m * CHANNELS : (m + 1) * CHANNELS, :
            ]
    run(net1, 3)
    run(net1)
    finish(net1)
    start_b()
    other_a()
    pass_a(2, 1)
    pass_a(0, 1)
    add_a(0, [0])
    add_b(0, [0])
    other_b()
    pass_b(2, 1)
    pass_b(0, 1)
    pass_a(2, 2)
    pass_a(1, 1)
    pass_a(0, 2)
    add_a(1, [0])
    pass_b(2, 2)
    pass_b(1, 1)
    pass_b(0, 2)
    add_a(0, [1, 7])
    add_b(1, [0])
    pass_a(2, 3)
    pass_a(1, 2)
    pass_a(0, 3)
    add_a(1, [1, 7])
    add_b(0, [1, 7])
    pass_b(2, 3)
    pass_b(1, 2)
    pass_b(0, 3)
    add_b(1, [1, 7])
    add_a(0, [2, 6])
    pass_a(2, 4)
    pass_a(1, 3)
    pass_a(0, 4)
    add_a(1, [2, 6])
    add_a(0, [3, 5])
    add_a(0, [4])
    add_b(0, [2, 6])
    pass_b(2, 4)
    pass_b(1, 3)
    pass_b(0, 4)
    add_b(1, [2, 6])
    add_b(0, [3, 5])
    add_b(0, [4])
    pass_a(1, 4)
    add_a(1, [3, 5])
    add_a(1, [4])
    end_a()
    pass_b(1, 4)
    add_b(1, [3, 5])
    add_b(1, [4])
    end_b()
    for c in started:
        c.wait_send()
    for c in results:
        c.wait()


def body(
    fields,
    wind_east,
    wind_north,
    diffusion,
    inflow_owner,
    inflow_cell,
    inflow_node,
    inflow_weight,
    encoder,
    sender_weight,
    receiver_weight,
    update_weight,
    decoder,
    edge_sender,
    edge_receiver,
    halo_rows,
    outflow_owner,
    outflow_node,
    outflow_cell,
    outflow_weight,
):
    vmem = pl.BlockSpec(memory_space=pltpu.VMEM)
    smem = pl.BlockSpec(memory_space=pltpu.SMEM)
    anywhere = pl.BlockSpec(memory_space=pl.ANY)
    half = (CHANNELS - HALF, NODES)
    scratch = [
        pltpu.VMEM((MEMBERS, CHANNELS * ROWS, COLS), F32),
        pltpu.VMEM((ROWS, FEATURES, COLS), F32),
        pltpu.VMEM((ROWS, FEATURES, COLS), F32),
        pltpu.VMEM((DSTEPS, MEMBERS, 2, CHANNELS, COLS), BF16),
        pltpu.VMEM((DSTEPS, MEMBERS, 2, CHANNELS, COLS), BF16),
        pltpu.VMEM((DSTEPS, MEMBERS, GROUP, COLS), BF16),
        pltpu.VMEM((DSTEPS, MEMBERS, 2, GROUP, COLS), BF16),
        pltpu.VMEM((FEATURES, CELLS), BF16),
        pltpu.VMEM((BLOCKS // 2, CELLS, 2 * ENTRIES), BF16),
        pltpu.VMEM((BLOCKS + 1, FEATURES, ENTRIES), BF16),
        pltpu.VMEM((BLOCKS + 1, NODES, ENTRIES), BF16),
        pltpu.VMEM((N_LON, 8, ENTRIES), F32),
        pltpu.VMEM((N_LON, 8, ENTRIES), F32),
        pltpu.VMEM((4, 8, 128), jnp.int32),
        pltpu.VMEM((N_LON, FEATURES, NODES), F32),
        pltpu.VMEM((MEMBERS, 3, 2, 4) + half, BF16),
        pltpu.VMEM((MEMBERS, 3, 2, 4) + half, BF16),
        pltpu.VMEM((MEMBERS, N_Z) + half, BF16),
        pltpu.VMEM((MEMBERS, N_Z) + half, BF16),
        pltpu.VMEM((MEMBERS, HALF, NODES), BF16),
        pltpu.VMEM((MEMBERS, HALF, NODES), BF16),
        pltpu.VMEM((MEMBERS, CHANNELS, NODES), F32),
        pltpu.VMEM((EDGES, 3 * NODES), BF16),
        pltpu.VMEM((NODES, EDGES), BF16),
        pltpu.VMEM((4, HCAP, NODES), BF16),
        pltpu.VMEM((CHANNELS, HID), BF16),
        pltpu.VMEM((LAYERS, HID, HID), BF16),
        pltpu.VMEM((LAYERS, HID, HID), BF16),
        pltpu.VMEM((LAYERS, HID, HID), BF16),
        pltpu.VMEM((CHANNELS, HID), BF16),
        pltpu.VMEM((MEMBERS, NODES, HID), F32),
        pltpu.VMEM((MEMBERS, 2 * NODES, HID), BF16),
        pltpu.VMEM((MEMBERS, LAYERS, 4, HCAP, HID), BF16),
        pltpu.VMEM((MEMBERS, LAYERS, NODES, HID), BF16),
        pltpu.VMEM((MEMBERS, EDGES, HID), F32),
        pltpu.VMEM((MEMBERS, EDGES, HID), BF16),
        pltpu.VMEM((N_LON, NODES, CELLS), BF16),
        pltpu.VMEM((MEMBERS, 2, N_Z, CHANNELS, NODES), BF16),
        pltpu.VMEM((MEMBERS, CHANNELS, CELLS), F32),
        pltpu.SMEM((N_LON * CAP,), jnp.int32),
        pltpu.VMEM((8, 128), jnp.int32),
        pltpu.SemaphoreType.DMA((9,)),
        pltpu.SemaphoreType.DMA((COPIES,)),
        pltpu.SemaphoreType.DMA((COPIES,)),
    ]
    result = pl.pallas_call(
        kernel,
        out_shape=jax.ShapeDtypeStruct((MEMBERS, CHANNELS * ROWS, COLS), F32),
        in_specs=[smem, smem, anywhere]
        + [vmem] * 6
        + [anywhere] * 5
        + [vmem] * 6,
        out_specs=anywhere,
        scratch_shapes=scratch,
        compiler_params=pltpu.CompilerParams(
            collective_id=0, has_side_effects=True, vmem_limit_bytes=VMEM_LIMIT
        ),
    )(
        inflow_owner.reshape(1, BLOCKS),
        outflow_owner.reshape(1, BLOCKS),
        fields.reshape(MEMBERS, CHANNELS * ROWS, COLS),
        wind_east,
        wind_north,
        diffusion,
        inflow_cell,
        inflow_node,
        inflow_weight,
        encoder,
        sender_weight,
        receiver_weight,
        update_weight,
        decoder.T,
        edge_sender,
        edge_receiver,
        halo_rows,
        outflow_node,
        outflow_cell,
        outflow_weight,
    )
    return result.reshape(MEMBERS, CHANNELS, ROWS, COLS)


def solution(mesh):
    placed = (
        P("member", None, "lat", "lon"),
        P("lat", "lon"),
        P("lat", "lon"),
        P("lat", "lon"),
        P(("lat", "lon"), None),
        P(("lat", "lon"), None),
        P(("lat", "lon"), None),
        P(("lat", "lon"), None),
        P(),
        P(),
        P(),
        P(),
        P(),
        P("lat", "lon", None),
        P("lat", "lon", None),
        P("lat", "lon", None, None),
        P(("lat", "lon"), None),
        P(("lat", "lon"), None),
        P(("lat", "lon"), None),
        P(("lat", "lon"), None),
    )
    return jax.shard_map(
        body, mesh=mesh, in_specs=placed, out_specs=P("member", None, "lat", "lon"), check_vma=False
    )
```
